32 devices in a mesh: dp: 16 (over z, x, core), tensor: 2 (over y).
Axes of the slice: x: 2, y: 2, z: 4, core: 2. Of those that a mesh axis runs over, the one named last changes fastest.
Arguments:
- query_rows: bfloat16 [6144, 5120], P('dp', 'tensor'), may hold values from -128 to 128
- key_rows: bfloat16 [6144, 5120], P('dp', 'tensor'), may hold values from -5 to 5
- value_rows: bfloat16 [6144, 5120], P('dp', 'tensor'), may hold values from -12 to 12
- action_mask: int32 [16, 384], P('dp'), may hold values from 0 to 1, as said below
- residual: bfloat16 [6144, 5120], P('dp', 'tensor'), may hold values from -100 to 100
- out_weight: bfloat16 [5120, 5120], P(None, 'tensor'), may hold values from -0.078125 to 0.078125
- norm_gain: float32 [5120], P('tensor'), may hold values from 0.1 to 1.9
- upstream: bfloat16 [6144, 5120], P('dp', 'tensor'), may hold values from -6 to 6
- residual_grad: bfloat16 [6144, 5120], P('dp', 'tensor'), may hold values from -2 to 2
Outputs:
- layer_out: bfloat16 [6144, 5120], P('dp', 'tensor')
- grad_residual: bfloat16 [6144, 5120], P('dp', 'tensor')
- grad_query: bfloat16 [6144, 5120], P('dp', 'tensor')
- grad_key: bfloat16 [6144, 5120], P('dp', 'tensor')
- grad_value: bfloat16 [6144, 5120], P('dp', 'tensor')
- grad_out_weight: float32 [5120, 5120], P('dp', 'tensor')
- grad_gain: float32 [5120], P('tensor')
The draws below stay inside these ranges and needn't reach their ends.
Inputs may be any that keep to these rules, and one draw needn't show every extreme that they name: `action_mask`: each row is a run of zeros followed by a run of ones; the ones number 1 to 192.
All inputs are finite; a program needn't handle non-finite values.
Results may differ from the reference program's by a relative error of at most 0.015.
Values may be sent and summed in bfloat16 or wider, within the bound.
A program may use at most 192 MiB of HBM per device.

```python
import jax
import jax.numpy as jnp
from jax import lax

D = 5120
HEADS = 40
HEAD_DIM = 128
LEN = 384
SEQS = 16
TOKENS = 6144


def attention_inputs(key):
    base_key = jax.random.fold_in(key, 17)
    key_query, key_key = jax.random.split(base_key, 2)
    shape = (SEQS, LEN, HEADS, HEAD_DIM)
    query_draw = jax.random.truncated_normal(key_query, -4.0, 4.0, shape, jnp.float32)
    key_draw = jax.random.truncated_normal(key_key, -4.0, 4.0, shape, jnp.float32)
    width = HEADS * HEAD_DIM
    return (query_draw.reshape(TOKENS, width), key_draw.reshape(TOKENS, width))


def draw_query_rows(key, part):
    return attention_inputs(key)[0].astype(jnp.bfloat16)


def draw_key_rows(key, part):
    return attention_inputs(key)[1].astype(jnp.bfloat16)


def draw_residual(key, part):
    key_base, key_rows = jax.random.split(jax.random.fold_in(key, 29), 2)
    columns = jnp.arange(D).astype(jnp.float32)
    column_scale = 10.0 ** (0.5 * columns / (D - 1))
    row_scale = jnp.exp(jax.random.uniform(key_rows, (TOKENS, 1), jnp.float32, jnp.log(0.5), jnp.log(5.0)))
    base = jax.random.truncated_normal(key_base, -5.0, 5.0, (TOKENS, D), jnp.float32)
    return (base * row_scale * column_scale[None, :]).astype(jnp.bfloat16)


def draw_action_mask(key, part):
    actions = jax.random.randint(jax.random.fold_in(key, 41), (SEQS,), 1, LEN // 2 + 1)
    position = jnp.arange(LEN)
    return (position[None, :] >= LEN - actions[:, None]).astype(jnp.int32)


def spiked(drawn, stream_key, source, target, parts, factor):
    def block_of(dim):
        return (jnp.arange(drawn.shape[dim]) // (drawn.shape[dim] // parts)).reshape((-1,) + (1,) * (drawn.ndim - 1 - dim))

    first = jax.random.permutation(stream_key, parts)[block_of(target)]
    far = (block_of(target) + parts // 2) % parts
    return jnp.where((block_of(source) == first) | (block_of(source) == far), factor * drawn, drawn)


def steps_of(rng, extent, shards, least, high):
    def one(dim, parts):
        heights = jax.random.uniform(jax.random.fold_in(jax.random.fold_in(rng, 6), dim), (parts,), jnp.float32, least / len(shards), high / len(shards))
        return jnp.repeat(jnp.exp(heights), extent[dim] // parts).reshape((-1,) + (1,) * (len(extent) - dim - 1))

    factor_of = one(*shards[0])
    for cut in shards[1:]:
        factor_of = factor_of * one(*cut)
    return factor_of


def centred(own_key, extent, scale, reach, cuts=(), held_as=jnp.bfloat16):
    result = scale * jax.random.normal(own_key, extent, jnp.float32)
    if cuts:
        result = result * steps_of(own_key, extent, cuts, -0.22, 0.18)
    return jnp.clip(result, -reach, reach).astype(held_as)


def gaussian_with(key, shape, scale, most, shards, heavy, kind=jnp.bfloat16):
    drawn = scale * jax.random.normal(key, shape, jnp.float32)
    if shards:
        drawn = drawn * steps_of(key, shape, shards, -0.22, 0.18)
    return jnp.clip(spiked(drawn, jax.random.fold_in(key, 3), *heavy), -most, most).astype(kind)


def setup_inputs(seed: int = 0) -> dict:
    key_of = jax.random.split(jax.random.key(seed), 10)
    return {
        "query_rows": draw_query_rows(jax.random.fold_in(key_of[9], 71), 0),
        "key_rows": draw_key_rows(jax.random.fold_in(key_of[9], 71), 0),
        "value_rows": centred(key_of[2], (TOKENS, HEADS * HEAD_DIM), 2.0, 12.0, ((0, 16), (1, 2))),
        "action_mask": draw_action_mask(jax.random.fold_in(key_of[9], 71), 0),
        "residual": draw_residual(jax.random.fold_in(key_of[9], 71), 0),
        "out_weight": centred(key_of[5], (D, HEADS * HEAD_DIM), (HEADS * HEAD_DIM) ** -0.5, 0.078125, ((1, 2),)),
        "norm_gain": jnp.clip(1.0 + 0.18 * jax.random.normal(key_of[6], (D,), jnp.float32), 0.1, 1.9),
        "upstream": gaussian_with(key_of[7], (TOKENS, D), 1.0, 6.0, ((0, 16), (1, 2)), (0, 1, 16, 2.0)),
        "residual_grad": centred(key_of[8], (TOKENS, D), 0.3, 2.0, ((0, 16), (1, 2))),
    }


epsilon = 1e-05

def visible(mask_row):
    position = jnp.arange(mask_row.shape[0])
    causal = position[None, :] <= position[:, None]
    observe = mask_row == 0
    return causal | observe[:, None] & observe[None, :]

def softmax_rows(query_heads, keyset, allowed):
    scores = jnp.einsum('qhd,khd->hqk', query_heads.astype(jnp.float32), keyset.astype(jnp.float32)) * HEAD_DIM ** (-0.5)
    masked = jnp.where(allowed[None], scores, -jnp.inf)
    row_top = lax.optimization_barrier(jnp.max(masked, axis=-1, keepdims=True))
    weights = jnp.exp(masked - row_top)
    return weights / lax.optimization_barrier(jnp.sum(weights, axis=-1, keepdims=True))

def split_heads(rows):
    return rows.reshape(LEN, HEADS, HEAD_DIM)

def forward_seq(inputs):
    query_seq, key_seq, value_seq, mask_row = inputs
    chances = softmax_rows(split_heads(query_seq), split_heads(key_seq), visible(mask_row))
    chances_low = lax.optimization_barrier(chances.astype(jnp.bfloat16)).astype(jnp.float32)
    attended = jnp.einsum('hqk,khd->qhd', chances_low, split_heads(value_seq).astype(jnp.float32))
    return attended.astype(jnp.bfloat16).reshape(LEN, HEADS * HEAD_DIM)

def backward_seq(inputs):
    query_seq, key_seq, value_seq, mask_row, grad_seq = inputs
    query_heads = split_heads(query_seq)
    key_heads = split_heads(key_seq)
    chances = softmax_rows(query_heads, key_heads, visible(mask_row))
    chances_low = lax.optimization_barrier(chances.astype(jnp.bfloat16)).astype(jnp.float32)
    grad_heads = split_heads(grad_seq).astype(jnp.float32)
    grad_value = jnp.einsum('hqk,qhd->khd', chances_low, grad_heads).astype(jnp.bfloat16)
    grad_chances = jnp.einsum('qhd,khd->hqk', grad_heads, split_heads(value_seq).astype(jnp.float32))
    row_delta = lax.optimization_barrier(jnp.sum(chances * grad_chances, axis=-1, keepdims=True))
    grad_scores = (chances * (grad_chances - row_delta) * HEAD_DIM ** (-0.5)).astype(jnp.bfloat16)
    grad_scores = lax.optimization_barrier(grad_scores).astype(jnp.float32)
    grad_query = jnp.einsum('hqk,khd->qhd', grad_scores, key_heads.astype(jnp.float32)).astype(jnp.bfloat16)
    grad_key = jnp.einsum('hqk,qhd->khd', grad_scores, query_heads.astype(jnp.float32)).astype(jnp.bfloat16)
    width = HEADS * HEAD_DIM
    return (grad_query.reshape(LEN, width), grad_key.reshape(LEN, width), grad_value.reshape(LEN, width))

def reference(query_rows, key_rows, value_rows, action_mask, residual, out_weight, norm_gain, upstream, residual_grad):
    width = HEADS * HEAD_DIM
    query_seq = query_rows.reshape(SEQS, LEN, width)
    key_seq = key_rows.reshape(SEQS, LEN, width)
    value_seq = value_rows.reshape(SEQS, LEN, width)
    attended = lax.map(forward_seq, (query_seq, key_seq, value_seq, action_mask)).reshape(TOKENS, width)
    projected = jnp.dot(attended, out_weight.T, preferred_element_type=jnp.float32)
    layer_out = (projected + residual.astype(jnp.float32)).astype(jnp.bfloat16)
    out_float = layer_out.astype(jnp.float32)
    row_rms = jnp.sqrt(lax.optimization_barrier(jnp.mean(out_float * out_float, axis=1, keepdims=True)) + epsilon)
    normed = out_float / row_rms
    scaled = upstream.astype(jnp.float32) * norm_gain[None, :]
    row_inner = lax.optimization_barrier(jnp.sum(scaled * out_float, axis=1, keepdims=True)) / (row_rms * D)
    grad_residual = (residual_grad.astype(jnp.float32) + (scaled - normed * row_inner) / row_rms).astype(jnp.bfloat16)
    grad_gain = lax.optimization_barrier(jnp.sum(upstream.astype(jnp.float32) * normed, axis=0))
    grad_out_weight = lax.dot_general(grad_residual, attended, (((0,), (0,)), ((), ())), preferred_element_type=jnp.float32)
    grad_attended = jnp.dot(grad_residual, out_weight, preferred_element_type=jnp.float32).astype(jnp.bfloat16)
    grad_seq = grad_attended.reshape(SEQS, LEN, width)
    grad_query, grad_key, grad_value = lax.map(backward_seq, (query_seq, key_seq, value_seq, action_mask, grad_seq))
    return (layer_out, grad_residual, grad_query.reshape(TOKENS, width), grad_key.reshape(TOKENS, width), grad_value.reshape(TOKENS, width), grad_out_weight, grad_gain)
```

```python
import functools

import jax
import jax.numpy as jnp
from jax import lax
from jax.experimental import pallas as pl
from jax.experimental.pallas import tpu as pltpu
from jax.sharding import PartitionSpec as P

HEAD_DIM = 128
LEN = 384

epsilon = 1e-05
SCALE = HEAD_DIM ** (-0.5)
NT = (((1,), (1,)), ((), ()))
TN = (((0,), (0,)), ((), ()))


def dot(a, b, dims):
    return lax.dot_general(a, b, dims, preferred_element_type=jnp.float32)


def forward_kernel(heads, observed_ref, query_ref, key_ref, value_ref, probs_ref, attended_ref):
    observed = observed_ref[pl.program_id(0)]
    row = lax.broadcasted_iota(jnp.int32, (LEN, LEN), 0)
    column = lax.broadcasted_iota(jnp.int32, (LEN, LEN), 1)
    allowed = column <= jnp.maximum(row, observed - 1)
    for head in range(heads):
        span = slice(head * HEAD_DIM, (head + 1) * HEAD_DIM)
        scores = dot(query_ref[:, span], key_ref[:, span], NT) * SCALE
        masked = jnp.where(allowed, scores, -jnp.inf)
        weights = jnp.exp(masked - jnp.max(masked, axis=1, keepdims=True))
        probs = weights * (1.0 / jnp.sum(weights, axis=1, keepdims=True))
        low = probs.astype(jnp.bfloat16)
        probs_ref[head] = low
        attended_ref[:, span] = jnp.dot(
            low, value_ref[:, span], preferred_element_type=jnp.float32
        ).astype(jnp.bfloat16)


def backward_kernel(
    heads, probs_ref, query_ref, key_ref, value_ref, cotangent_ref, query_out, key_out, value_out
):
    for head in range(heads):
        span = slice(head * HEAD_DIM, (head + 1) * HEAD_DIM)
        low = probs_ref[head]
        cotangent = cotangent_ref[:, span]
        value_out[:, span] = dot(low, cotangent, TN).astype(jnp.bfloat16)
        grad_probs = dot(cotangent, value_ref[:, span], NT)
        probs = low.astype(jnp.float32)
        delta = jnp.sum(probs * grad_probs, axis=1, keepdims=True)
        grad_scores = (probs * (grad_probs - delta) * SCALE).astype(jnp.bfloat16)
        query_out[:, span] = jnp.dot(
            grad_scores, key_ref[:, span], preferred_element_type=jnp.float32
        ).astype(jnp.bfloat16)
        key_out[:, span] = dot(grad_scores, query_ref[:, span], TN).astype(jnp.bfloat16)


def head_group(head_count):
    return max(size for size in range(1, 6) if head_count % size == 0)


def specs(heads):
    rows = pl.BlockSpec((LEN, heads * HEAD_DIM), lambda s, h: (s, h))
    square = pl.BlockSpec((None, heads, LEN, LEN), lambda s, h: (s, h, 0, 0))
    return rows, square


def attend(observed, query_rows, key_rows, value_rows):
    tok_rows, width = query_rows.shape
    head_count, seq_count = width // HEAD_DIM, tok_rows // LEN
    heads = head_group(head_count)
    rows, square = specs(heads)
    pairs = seq_count * head_count * LEN * LEN
    return pl.pallas_call(
        functools.partial(forward_kernel, heads),
        grid=(seq_count, head_count // heads),
        in_specs=[pl.BlockSpec(memory_space=pltpu.SMEM), rows, rows, rows],
        out_specs=[square, rows],
        out_shape=[
            jax.ShapeDtypeStruct((seq_count, head_count, LEN, LEN), jnp.bfloat16),
            jax.ShapeDtypeStruct((tok_rows, width), jnp.bfloat16),
        ],
        cost_estimate=pl.CostEstimate(
            flops=4 * pairs * HEAD_DIM,
            bytes_accessed=2 * pairs + 8 * tok_rows * width,
            transcendentals=pairs,
        ),
        name="attend",
    )(observed, query_rows, key_rows, value_rows)


def attend_backward(probs, query_rows, key_rows, value_rows, cotangent):
    tok_rows, width = query_rows.shape
    head_count, seq_count = width // HEAD_DIM, tok_rows // LEN
    heads = head_group(head_count)
    rows, square = specs(heads)
    pairs = seq_count * head_count * LEN * LEN
    return pl.pallas_call(
        functools.partial(backward_kernel, heads),
        grid=(seq_count, head_count // heads),
        in_specs=[square, rows, rows, rows, rows],
        out_specs=[rows, rows, rows],
        out_shape=[jax.ShapeDtypeStruct((tok_rows, width), jnp.bfloat16)] * 3,
        cost_estimate=pl.CostEstimate(
            flops=8 * pairs * HEAD_DIM,
            bytes_accessed=2 * pairs + 14 * tok_rows * width,
            transcendentals=0,
        ),
        name="attend_backward",
    )(probs, query_rows, key_rows, value_rows, cotangent)


MESH = pl.DeviceIdType.MESH


def trunk_kernel(
    groups,
    att_h,
    res_h,
    ups_h,
    rg_h,
    gain_ref,
    w_h,
    probs_h,
    q_h,
    k_h,
    v_h,
    lo_h,
    gr_h,
    gq_h,
    gk_h,
    gv_h,
    gw_h,
    gain_o,
    gath,
    att_v,
    ups_v,
    rg_v,
    theirs,
    arrived,
    lo_v,
    gr_v,
    turned,
    turned_other,
    other_v,
    pieces,
    sums_mine,
    sums_theirs,
    gain_v,
    mid_out,
    mid_in,
    load_sem,
    w_sem,
    p_sems,
    g_sems,
    s_sems,
    ag_sems,
    piece_sems,
    gain_sems,
    mid_sems,
    block_sem,
    fetch_sem,
    out_sem,
    final_sem,
):
    rows, width = att_v.shape
    model = 2 * width
    chips = 4
    part = width // chips
    own_rows = part // 2
    half = width // 2
    d = lax.axis_index("dp")
    t = lax.axis_index("tensor")
    c = d % 2
    x = (d // 2) % 2
    zp = (d // 4) % 2
    zh = d // 8

    def device(zh_, zp_, x_, c_, t_):
        return (((zh_ * 2 + zp_) * 2 + x_) * 2 + c_, t_)

    y_peer = (d, 1 - t)
    x_peer = device(zh, zp, 1 - x, c, t)
    z_peer = device(zh, 1 - zp, x, c, t)
    core_peer = device(zh, zp, x, 1 - c, t)
    mid_peer = device(1 - zh, zp, x, c, t)

    def remote(src, dst, sems, index, target):
        return pltpu.make_async_remote_copy(
            src_ref=src,
            dst_ref=dst,
            send_sem=sems.at[(0,) + index],
            recv_sem=sems.at[(1,) + index],
            device_id=target,
            device_id_type=MESH,
        )

    barrier = pltpu.get_barrier_semaphore()
    for r in range(1, groups):
        pl.semaphore_signal(barrier, inc=1, device_id=((d + r) % groups, t), device_id_type=MESH)
    pl.semaphore_signal(barrier, inc=1, device_id=y_peer, device_id_type=MESH)

    def gather(src, slot, side, target):
        cols = slice(side * half, (side + 1) * half)
        return remote(src.at[:, cols], gath.at[slot, :, cols], ag_sems, (slot, side), target)

    def piece(kind, source, k, dc):
        kz, kx = k // 2, k % 2
        dz = zp + kz - 2 * zp * kz
        dx = x + kx - 2 * x * kx
        core = c + dc - 2 * c * dc
        delta = dz * 4 + dx * 2 + dc
        src = source.at[k, pl.ds(core * own_rows, own_rows), :]
        dst = pieces.at[kind, :, pl.ds(pl.multiple_of(delta * rows, 128), rows)]
        far = remote(src, dst, piece_sems, (kind, delta), device(zh, kz, kx, core, t))
        if dc == 1:
            far.start()
        else:

            @pl.when(dz + dx > 0)
            def _():
                far.start()

            @pl.when(dz + dx == 0)
            def _():
                pltpu.make_async_copy(src, pieces.at[kind, :, 0:rows], piece_sems.at[1, kind, 0]).start()

    def projection(wp, res_v):
        def w_load(side, k):
            start = pl.multiple_of(side * width + k * part, part)
            return pltpu.make_async_copy(w_h.at[pl.ds(start, part), :], wp.at[k], w_sem.at[k])

        att_load = pltpu.make_async_copy(att_h, att_v, load_sem.at[0])
        att_load.start()
        for k in range(chips):
            w_load(1 - t, k).start()
        later = [
            pltpu.make_async_copy(a, b, load_sem.at[i + 1])
            for i, (a, b) in enumerate(((res_h, res_v), (ups_h, ups_v), (rg_h, rg_v)))
        ]
        for copy in later:
            copy.start()
        pl.semaphore_wait(barrier, groups)
        gather(att_h, 4, 0, z_peer).start()
        gather(att_h, 2, 1, x_peer).start()
        gather(att_h, 4, 1, z_peer).start()
        gather(att_h, 2, 0, x_peer).start()
        for side in (0, 1):
            gather(att_h, 1, side, core_peer).start()
        att_load.wait()

        def give(k, carry):
            w_load(1 - t, k).wait()
            theirs[k] = dot(att_v[...], wp[k], NT).astype(jnp.bfloat16)
            remote(theirs.at[k], arrived.at[k], p_sems, (k,), y_peer).start()
            w_load(t, k).start()
            return carry

        lax.fori_loop(0, chips, give, 0)
        for copy in later:
            copy.wait()

        def take(k, carry):
            squares, inner = carry
            cols = pl.ds(pl.multiple_of(k * part, 128), part)
            w_load(t, k).wait()
            own = dot(att_v[...], wp[k], NT)
            remote(theirs.at[k], arrived.at[k], p_sems, (k,), y_peer).wait()
            total = own + arrived[k].astype(jnp.float32)
            low = (total + res_v[:, cols].astype(jnp.float32)).astype(jnp.bfloat16)
            lo_v[:, cols] = low
            out = low.astype(jnp.float32)
            scaled = ups_v[:, cols].astype(jnp.float32) * gain_ref[:, cols]
            squares = squares + jnp.sum(out * out, axis=1, keepdims=True)
            inner = inner + jnp.sum(scaled * out, axis=1, keepdims=True)
            return squares, inner

        zero = jnp.zeros((rows, 1), jnp.float32)
        carry = lax.fori_loop(0, 2, take, (zero, zero))
        gather(att_h, 4, 0, z_peer).wait_recv()
        gather(gath.at[4], 6, 0, x_peer).start()
        gather(att_h, 2, 1, x_peer).wait_recv()
        gather(gath.at[2], 6, 1, z_peer).start()
        squares, inner = lax.fori_loop(2, chips, take, carry)
        lane = lax.broadcasted_iota(jnp.int32, (rows, 128), 1)
        packed = jnp.where(lane == 0, squares, jnp.where(lane == 1, inner, 0.0))
        sums_mine[...] = jnp.transpose(packed)[0:8]

    pl.run_scoped(
        projection,
        pltpu.VMEM((chips, part, width), jnp.bfloat16),
        pltpu.VMEM((rows, width), jnp.bfloat16),
    )
    exchange = remote(sums_mine, sums_theirs, s_sems, (0,), y_peer)
    exchange.start()
    lo_out = pltpu.make_async_copy(lo_v, lo_h, load_sem.at[0])
    lo_out.start()
    exchange.wait()
    both = sums_mine[...] + sums_theirs[...]
    wide = jnp.transpose(jnp.concatenate([both, jnp.zeros((120, rows), jnp.float32)], axis=0))
    squares, inner = wide[:, 0:1], wide[:, 1:2]
    rms = jnp.sqrt(squares / model + epsilon)
    inverse = 1.0 / rms
    row_inner = inner / (rms * model)
    slope = row_inner * inverse

    def normalise(k, carry):
        cols = pl.ds(pl.multiple_of(k * part, 128), part)
        out = lo_v[:, cols].astype(jnp.float32)
        ups = ups_v[:, cols].astype(jnp.float32)
        scaled = ups * gain_ref[:, cols]
        grad = (rg_v[:, cols].astype(jnp.float32) + (scaled - out * slope) * inverse).astype(jnp.bfloat16)
        gr_v[:, cols] = grad
        turned[k] = jnp.transpose(grad.astype(jnp.float32)).astype(jnp.bfloat16)
        gain_v[d, :, cols] = jnp.sum(ups * (out * inverse), axis=0, keepdims=True)
        remote(turned.at[k], turned_other.at[k], g_sems, (k,), y_peer).start()
        for dc in (0, 1):
            piece(0, turned, k, dc)
        return carry

    lax.fori_loop(0, chips, normalise, 0)
    gr_out = pltpu.make_async_copy(gr_v, gr_h, load_sem.at[1])
    gr_out.start()

    def gain_copy(r, sender):
        return remote(gain_v.at[sender], gain_v.at[sender], gain_sems, (r,), ((d + r) % groups, t))

    for r in range(1, groups):
        gain_copy(r, d).start()
    for side in (0, 1):
        if side == 1:
            gather(att_h, 4, 1, z_peer).wait_recv()
        gather(gath.at[4], 5, side, core_peer).start()
        if side == 0:
            gather(att_h, 2, 0, x_peer).wait_recv()
        gather(gath.at[2], 3, side, core_peer).start()

    def pass_on(k, carry):
        remote(turned.at[k], turned_other.at[k], g_sems, (k,), y_peer).wait()
        for dc in (0, 1):
            piece(1, turned_other, k, dc)
        cols = pl.ds(pl.multiple_of(k * part, 128), part)
        other_v[:, cols] = jnp.transpose(turned_other[k].astype(jnp.float32)).astype(jnp.bfloat16)
        return carry

    lax.fori_loop(0, 2, pass_on, 0)
    for side in (0, 1):
        gather(gath.at[4], 6, side, x_peer).wait_recv()
        gather(gath.at[6], 7, side, core_peer).start()
    lax.fori_loop(2, chips, pass_on, 0)
    for slot in (1, 3, 5, 7):
        for side in (0, 1):
            gather(att_h, slot, side, core_peer).wait_recv()

    blocks = width // part
    keeps_first = (zh + t) % 2 == 0

    def finish(kept, att_b):
        def block_load(cb, slot):
            cols = pl.ds(pl.multiple_of(cb * part, 128), part)
            copies = [
                pltpu.make_async_copy(
                    att_h.at[:, cols], att_b.at[slot, 0:rows, :], block_sem.at[slot, 0]
                )
            ]
            for delta in range(1, 8):
                copies.append(
                    pltpu.make_async_copy(
                        gath.at[delta, :, cols],
                        att_b.at[slot, delta * rows : (delta + 1) * rows, :],
                        block_sem.at[slot, delta],
                    )
                )
            return copies

        def mid_copy(cb):
            return remote(mid_out.at[cb], mid_in.at[cb], mid_sems, (cb,), mid_peer)

        for copy in block_load(0, 0):
            copy.start()
        for kind in (0, 1):
            for delta in range(8):
                pltpu.make_async_copy(
                    turned.at[0, 0:own_rows, :],
                    pieces.at[kind, :, delta * rows : (delta + 1) * rows],
                    piece_sems.at[1, kind, delta],
                ).wait()
            keeps = keeps_first if kind == 0 else jnp.logical_not(keeps_first)

            def product(cb, carry, kind=kind, keeps=keeps):
                slot = cb % 2
                if kind == 0:
                    for copy in block_load((cb + 1) % blocks, 1 - slot):
                        copy.start()
                else:

                    @pl.when(cb + 1 < blocks)
                    def _():
                        for copy in block_load(cb + 1, 1 - slot):
                            copy.start()

                for copy in block_load(cb, slot):
                    copy.wait()
                value = jnp.dot(pieces[kind], att_b[slot], preferred_element_type=jnp.float32)

                @pl.when(keeps)
                def _():
                    kept[cb] = value

                @pl.when(jnp.logical_not(keeps))
                def _():
                    mid_out[cb] = value.astype(jnp.bfloat16)
                    mid_copy(cb).start()

                return carry

            lax.fori_loop(0, blocks, product, 0)

        def attention(pb, qb, kb, vb, wc, ob):
            steps = width // (2 * HEAD_DIM)

            def fetch(i, slot):
                cols = pl.ds(pl.multiple_of(i * 2 * HEAD_DIM, 128), 2 * HEAD_DIM)
                pairs = (
                    (probs_h.at[pl.ds(2 * i, 2)], pb),
                    (q_h.at[:, cols], qb),
                    (k_h.at[:, cols], kb),
                    (v_h.at[:, cols], vb),
                    (w_h.at[:, cols], wc),
                )
                return [
                    pltpu.make_async_copy(a, b.at[slot], fetch_sem.at[slot, j])
                    for j, (a, b) in enumerate(pairs)
                ]

            def emit(i, slot):
                cols = pl.ds(pl.multiple_of(i * 2 * HEAD_DIM, 128), 2 * HEAD_DIM)
                return [
                    pltpu.make_async_copy(ob.at[slot, j], b.at[:, cols], out_sem.at[slot, j])
                    for j, b in enumerate((gq_h, gk_h, gv_h))
                ]

            for copy in fetch(0, 0):
                copy.start()

            def step(i, carry):
                slot = i % 2

                @pl.when(i + 1 < steps)
                def _():
                    for copy in fetch(i + 1, 1 - slot):
                        copy.start()

                for copy in fetch(i, slot):
                    copy.wait()

                @pl.when(i >= 2)
                def _():
                    for copy in emit(i - 2, slot):
                        copy.wait()

                mine = wc[slot, pl.ds(pl.multiple_of(t * width, 128), width), :]
                other = wc[slot, pl.ds(pl.multiple_of((1 - t) * width, 128), width), :]
                cotangents = (
                    jnp.dot(gr_v[...], mine, preferred_element_type=jnp.float32)
                    + jnp.dot(other_v[...], other, preferred_element_type=jnp.float32)
                ).astype(jnp.bfloat16)
                for j in range(2):
                    span = slice(j * HEAD_DIM, (j + 1) * HEAD_DIM)
                    low = pb[slot, j]
                    cotangent = cotangents[:, span]
                    ob[slot, 2, :, span] = dot(low, cotangent, TN).astype(jnp.bfloat16)
                    grad_probs = dot(cotangent, vb[slot, :, span], NT)
                    probs = low.astype(jnp.float32)
                    delta = jnp.sum(probs * grad_probs, axis=1, keepdims=True)
                    grad_scores = (probs * (grad_probs - delta) * SCALE).astype(jnp.bfloat16)
                    ob[slot, 0, :, span] = jnp.dot(
                        grad_scores, kb[slot, :, span], preferred_element_type=jnp.float32
                    ).astype(jnp.bfloat16)
                    ob[slot, 1, :, span] = dot(grad_scores, qb[slot, :, span], TN).astype(
                        jnp.bfloat16
                    )
                for copy in emit(i, slot):
                    copy.start()
                return carry

            lax.fori_loop(0, steps, step, 0)
            for i in (steps - 2, steps - 1):
                for copy in emit(i, i % 2):
                    copy.wait()

        two = 2 * HEAD_DIM
        pl.run_scoped(
            attention,
            pltpu.VMEM((2, 2, rows, rows), jnp.bfloat16),
            pltpu.VMEM((2, rows, two), jnp.bfloat16),
            pltpu.VMEM((2, rows, two), jnp.bfloat16),
            pltpu.VMEM((2, rows, two), jnp.bfloat16),
            pltpu.VMEM((2, model, two), jnp.bfloat16),
            pltpu.VMEM((2, 3, rows, two), jnp.bfloat16),
        )
        for r in range(1, groups):
            gain_copy(r, (d + groups - r) % groups).wait()
        total = gain_v[0]
        for i in range(1, groups):
            total = total + gain_v[i]
        gain_o[...] = total

        def close(cb, carry):
            mid_copy(cb).wait()
            kept[cb] = kept[cb] + mid_in[cb].astype(jnp.float32)
            cols = pl.ds(pl.multiple_of(cb * part, 128), part)
            pltpu.make_async_copy(kept.at[cb], gw_h.at[:, cols], final_sem.at[cb]).start()
            return carry

        lax.fori_loop(0, blocks, close, 0)
        for cb in range(blocks):
            cols = slice(cb * part, (cb + 1) * part)
            pltpu.make_async_copy(kept.at[cb], gw_h.at[:, cols], final_sem.at[cb]).wait()

    pl.run_scoped(
        finish,
        pltpu.VMEM((blocks, own_rows, part), jnp.float32),
        pltpu.VMEM((2, 8 * rows, part), jnp.bfloat16),
    )
    lo_out.wait()
    gr_out.wait()
    for slot in range(1, 8):
        for side in (0, 1):
            gather(att_h, slot, side, core_peer).wait_send()
    for kind in (0, 1):
        for delta in range(1, 8):
            remote(
                turned.at[0, 0:own_rows, :],
                pieces.at[kind, :, 0:rows],
                piece_sems,
                (kind, delta),
                core_peer,
            ).wait_send()


def trunk(groups, att, res, ups, rg, gain, weight, probs, q, k, v):
    rows, width = att.shape
    model = weight.shape[0]
    chips = 4
    part = width // chips
    own_rows = part // 2
    anywhere = pl.BlockSpec(memory_space=pl.ANY)
    local = pl.BlockSpec(memory_space=pltpu.VMEM)
    low = jnp.bfloat16
    act = jax.ShapeDtypeStruct((rows, width), low)
    dma = pltpu.SemaphoreType.DMA
    return pl.pallas_call(
        functools.partial(trunk_kernel, groups),
        in_specs=[anywhere] * 4 + [local] + [anywhere] * 5,
        out_specs=[anywhere] * 6 + [local, anywhere],
        out_shape=[act] * 5
        + [
            jax.ShapeDtypeStruct((own_rows, width), jnp.float32),
            jax.ShapeDtypeStruct((1, width), jnp.float32),
            jax.ShapeDtypeStruct((8, rows, width), low),
        ],
        scratch_shapes=[
            pltpu.VMEM((rows, width), low),
            pltpu.VMEM((rows, width), low),
            pltpu.VMEM((rows, width), low),
            pltpu.VMEM((chips, rows, part), low),
            pltpu.VMEM((chips, rows, part), low),
            pltpu.VMEM((rows, width), low),
            pltpu.VMEM((rows, width), low),
            pltpu.VMEM((chips, part, rows), low),
            pltpu.VMEM((chips, part, rows), low),
            pltpu.VMEM((rows, width), low),
            pltpu.VMEM((2, own_rows, 8 * rows), low),
            pltpu.VMEM((8, rows), jnp.float32),
            pltpu.VMEM((8, rows), jnp.float32),
            pltpu.VMEM((groups, 1, width), jnp.float32),
            pltpu.VMEM((chips, own_rows, part), low),
            pltpu.VMEM((chips, own_rows, part), low),
            dma((4,)),
            dma((chips,)),
            dma((2, chips)),
            dma((2, chips)),
            dma((2, 1)),
            dma((2, 8, 2)),
            dma((2, 2, 8)),
            dma((2, groups)),
            dma((2, chips)),
            dma((2, 8)),
            dma((2, 5)),
            dma((2, 3)),
            dma((chips,)),
        ],
        compiler_params=pltpu.CompilerParams(
            collective_id=0, has_side_effects=True, vmem_limit_bytes=66 * 1000 * 1000
        ),
        name="trunk",
    )(att, res, ups, rg, gain, weight, probs, q, k, v)


def sum_groups(groups, value):
    if groups & (groups - 1):
        return lax.psum(value, "dp")
    bit = 1
    while bit < groups:
        value = value + lax.ppermute(value, "dp", [(i, i ^ bit) for i in range(groups)])
        bit *= 2
    return value


def shards(
    groups,
    tensor_size,
    query_rows,
    key_rows,
    value_rows,
    action_mask,
    residual,
    out_weight,
    norm_gain,
    upstream,
    residual_grad,
):
    model_width = out_weight.shape[0]
    own_width = residual.shape[1]
    pair = tensor_size == 2
    swap = [(0, 1), (1, 0)]
    mine = lax.axis_index("tensor")

    def weight_rows(index):
        return lax.dynamic_slice_in_dim(out_weight, index * own_width, own_width, 0)

    def sum_pair(value):
        if pair:
            return value + lax.ppermute(value, "tensor", swap)
        return lax.psum(value, "tensor")

    observed = jnp.sum((action_mask == 0).astype(jnp.int32), axis=1)
    probs, attended = attend(observed, query_rows, key_rows, value_rows)
    if pair and groups == 16 and attended.shape[0] == LEN:
        out = trunk(
            groups,
            attended,
            residual,
            upstream,
            residual_grad,
            norm_gain[None, :],
            out_weight,
            probs[0],
            query_rows,
            key_rows,
            value_rows,
        )
        return (*out[:6], out[6][0])
    attended_all = lax.all_gather(attended, "dp", axis=0, tiled=True)
    if pair:
        theirs = dot(attended, weight_rows(1 - mine), NT).astype(jnp.bfloat16)
        arriving = lax.ppermute(theirs, "tensor", swap)
        own = dot(attended, weight_rows(mine), NT)
        own_sum = own + arriving.astype(jnp.float32)
    else:
        own_sum = lax.psum_scatter(
            dot(attended, out_weight, NT), "tensor", scatter_dimension=1, tiled=True
        )
    layer_out = (own_sum + residual.astype(jnp.float32)).astype(jnp.bfloat16)
    out_float = layer_out.astype(jnp.float32)
    upstream_float = upstream.astype(jnp.float32)
    scaled = upstream_float * norm_gain[None, :]
    sums = sum_pair(
        jnp.stack([jnp.sum(out_float * out_float, axis=1), jnp.sum(scaled * out_float, axis=1)])
    )
    row_rms = jnp.sqrt(sums[0] / model_width + epsilon)[:, None]
    normed = out_float / row_rms
    row_inner = sums[1][:, None] / (row_rms * model_width)
    grad_residual = (
        residual_grad.astype(jnp.float32) + (scaled - normed * row_inner) / row_rms
    ).astype(jnp.bfloat16)
    if pair:
        other = lax.ppermute(grad_residual, "tensor", swap)
        first = mine == 0
        low_half = jnp.where(first, grad_residual, other)
        high_half = jnp.where(first, other, grad_residual)
        grad_full = jnp.concatenate([low_half, high_half], axis=1)
        grad_attended = jnp.dot(
            grad_residual, weight_rows(mine), preferred_element_type=jnp.float32
        ) + jnp.dot(other, weight_rows(1 - mine), preferred_element_type=jnp.float32)
    else:
        grad_full = lax.all_gather(grad_residual, "tensor", axis=1, tiled=True)
        grad_attended = jnp.dot(grad_full, out_weight, preferred_element_type=jnp.float32)
    grad_attended = grad_attended.astype(jnp.bfloat16)
    received = lax.all_to_all(grad_full, "dp", split_axis=1, concat_axis=0, tiled=True)
    gain_part = jnp.sum(upstream_float * normed, axis=0)
    grad_query, grad_key, grad_value = attend_backward(
        probs, query_rows, key_rows, value_rows, grad_attended
    )
    grad_query, gain_part = lax.optimization_barrier((grad_query, gain_part))
    grad_gain = sum_groups(groups, gain_part)
    grad_out_weight = dot(received, attended_all, TN)
    return layer_out, grad_residual, grad_query, grad_key, grad_value, grad_out_weight, grad_gain


def solution(mesh):
    rows = P("dp", "tensor")
    return jax.shard_map(
        functools.partial(shards, mesh.shape["dp"], mesh.shape["tensor"]),
        mesh=mesh,
        in_specs=(
            rows,
            rows,
            rows,
            P("dp", None),
            rows,
            P(None, "tensor"),
            P("tensor"),
            rows,
            rows,
        ),
        out_specs=(rows, rows, rows, rows, rows, rows, P("tensor")),
        check_vma=False,
    )
```

```python
import functools

import jax
import jax.numpy as jnp
from jax import lax
from jax.experimental import pallas as pl
from jax.experimental.pallas import tpu as pltpu
from jax.sharding import PartitionSpec as P

HEAD_DIM = 128
LEN = 384

epsilon = 1e-05
SCALE = HEAD_DIM ** (-0.5)
NT = (((1,), (1,)), ((), ()))
TN = (((0,), (0,)), ((), ()))


def dot(a, b, dims):
    return lax.dot_general(a, b, dims, preferred_element_type=jnp.float32)


def forward_kernel(heads, observed_ref, query_ref, key_ref, value_ref, probs_ref, attended_ref):
    observed = observed_ref[pl.program_id(0)]
    row = lax.broadcasted_iota(jnp.int32, (LEN, LEN), 0)
    column = lax.broadcasted_iota(jnp.int32, (LEN, LEN), 1)
    allowed = column <= jnp.maximum(row, observed - 1)
    for head in range(heads):
        span = slice(head * HEAD_DIM, (head + 1) * HEAD_DIM)
        scores = dot(query_ref[:, span], key_ref[:, span], NT) * SCALE
        masked = jnp.where(allowed, scores, -jnp.inf)
        weights = jnp.exp(masked - jnp.max(masked, axis=1, keepdims=True))
        probs = weights * (1.0 / jnp.sum(weights, axis=1, keepdims=True))
        low = probs.astype(jnp.bfloat16)
        probs_ref[head] = low
        attended_ref[:, span] = jnp.dot(
            low, value_ref[:, span], preferred_element_type=jnp.float32
        ).astype(jnp.bfloat16)


def backward_kernel(
    heads, probs_ref, query_ref, key_ref, value_ref, cotangent_ref, query_out, key_out, value_out
):
    for head in range(heads):
        span = slice(head * HEAD_DIM, (head + 1) * HEAD_DIM)
        low = probs_ref[head]
        cotangent = cotangent_ref[:, span]
        value_out[:, span] = dot(low, cotangent, TN).astype(jnp.bfloat16)
        grad_probs = dot(cotangent, value_ref[:, span], NT)
        probs = low.astype(jnp.float32)
        delta = jnp.sum(probs * grad_probs, axis=1, keepdims=True)
        grad_scores = (probs * (grad_probs - delta) * SCALE).astype(jnp.bfloat16)
        query_out[:, span] = jnp.dot(
            grad_scores, key_ref[:, span], preferred_element_type=jnp.float32
        ).astype(jnp.bfloat16)
        key_out[:, span] = dot(grad_scores, query_ref[:, span], TN).astype(jnp.bfloat16)


def head_group(head_count):
    return max(size for size in range(1, 6) if head_count % size == 0)


def specs(heads):
    rows = pl.BlockSpec((LEN, heads * HEAD_DIM), lambda s, h: (s, h))
    square = pl.BlockSpec((None, heads, LEN, LEN), lambda s, h: (s, h, 0, 0))
    return rows, square


def attend(observed, query_rows, key_rows, value_rows):
    tok_rows, width = query_rows.shape
    head_count, seq_count = width // HEAD_DIM, tok_rows // LEN
    heads = head_group(head_count)
    rows, square = specs(heads)
    pairs = seq_count * head_count * LEN * LEN
    return pl.pallas_call(
        functools.partial(forward_kernel, heads),
        grid=(seq_count, head_count // heads),
        in_specs=[pl.BlockSpec(memory_space=pltpu.SMEM), rows, rows, rows],
        out_specs=[square, rows],
        out_shape=[
            jax.ShapeDtypeStruct((seq_count, head_count, LEN, LEN), jnp.bfloat16),
            jax.ShapeDtypeStruct((tok_rows, width), jnp.bfloat16),
        ],
        cost_estimate=pl.CostEstimate(
            flops=4 * pairs * HEAD_DIM,
            bytes_accessed=2 * pairs + 8 * tok_rows * width,
            transcendentals=pairs,
        ),
        name="attend",
    )(observed, query_rows, key_rows, value_rows)


def attend_backward(probs, query_rows, key_rows, value_rows, cotangent):
    tok_rows, width = query_rows.shape
    head_count, seq_count = width // HEAD_DIM, tok_rows // LEN
    heads = head_group(head_count)
    rows, square = specs(heads)
    pairs = seq_count * head_count * LEN * LEN
    return pl.pallas_call(
        functools.partial(backward_kernel, heads),
        grid=(seq_count, head_count // heads),
        in_specs=[square, rows, rows, rows, rows],
        out_specs=[rows, rows, rows],
        out_shape=[jax.ShapeDtypeStruct((tok_rows, width), jnp.bfloat16)] * 3,
        cost_estimate=pl.CostEstimate(
            flops=8 * pairs * HEAD_DIM,
            bytes_accessed=2 * pairs + 14 * tok_rows * width,
            transcendentals=0,
        ),
        name="attend_backward",
    )(probs, query_rows, key_rows, value_rows, cotangent)


MESH = pl.DeviceIdType.MESH


def trunk_kernel(
    groups,
    mask_ref,
    gain_h,
    res_h,
    ups_h,
    rg_h,
    w_h,
    q_h,
    k_h,
    v_h,
    lo_h,
    gr_h,
    gq_h,
    gk_h,
    gv_h,
    kept_h,
    mid_in,
    gain_o,
    gath,
    att_v,
    probs_v,
    ups_v,
    rg_v,
    gain_ref,
    theirs,
    arrived,
    lo_v,
    gr_v,
    turned,
    turned_other,
    other_v,
    wp,
    cotangent_sum,
    pieces,
    sums_mine,
    sums_theirs,
    gain_v,
    mid_out,
    load_sem,
    w_sem,
    p_sems,
    g_sems,
    s_sems,
    ag_sems,
    piece_sems,
    gain_sems,
    mid_sems,
    block_sem,
    fetch_sem,
    out_sem,
    final_sem,
):
    rows, width = att_v.shape
    model = 2 * width
    chips = 4
    part = width // chips
    own_rows = part // 2
    half = width // 2
    d = lax.axis_index("dp")
    t = lax.axis_index("tensor")
    c = d % 2
    x = (d // 2) % 2
    zp = (d // 4) % 2
    zh = d // 8

    def device(zh_, zp_, x_, c_, t_):
        return (((zh_ * 2 + zp_) * 2 + x_) * 2 + c_, t_)

    y_peer = (d, 1 - t)
    x_peer = device(zh, zp, 1 - x, c, t)
    z_peer = device(zh, 1 - zp, x, c, t)
    core_peer = device(zh, zp, x, 1 - c, t)
    mid_peer = device(1 - zh, zp, x, c, t)

    def remote(src, dst, sems, index, target):
        return pltpu.make_async_remote_copy(
            src_ref=src,
            dst_ref=dst,
            send_sem=sems.at[(0,) + index],
            recv_sem=sems.at[(1,) + index],
            device_id=target,
            device_id_type=MESH,
        )

    barrier = pltpu.get_barrier_semaphore()
    for r in range(1, groups):
        pl.semaphore_signal(barrier, inc=1, device_id=((d + r) % groups, t), device_id_type=MESH)
    pl.semaphore_signal(barrier, inc=1, device_id=y_peer, device_id_type=MESH)

    def gather(src, slot, side, target):
        cols = slice(side * half, (side + 1) * half)
        return remote(src.at[:, cols], gath.at[slot, :, cols], ag_sems, (slot, side), target)

    def piece(kind, source, k, dc):
        kz, kx = k // 2, k % 2
        dz = zp + kz - 2 * zp * kz
        dx = x + kx - 2 * x * kx
        core = c + dc - 2 * c * dc
        delta = dz * 4 + dx * 2 + dc
        src = source.at[k, pl.ds(core * own_rows, own_rows), :]
        dst = pieces.at[kind, :, pl.ds(pl.multiple_of(delta * rows, 128), rows)]
        far = remote(src, dst, piece_sems, (kind, delta), device(zh, kz, kx, core, t))
        if dc == 1:
            far.start()
        else:

            @pl.when(dz + dx > 0)
            def _():
                far.start()

            @pl.when(dz + dx == 0)
            def _():
                pltpu.make_async_copy(src, pieces.at[kind, :, 0:rows], piece_sems.at[1, kind, 0]).start()

    gain_ref[...] = jnp.reshape(gain_h[...], (1, width))
    two = 2 * HEAD_DIM
    steps = width // two

    def head_cols(i):
        return pl.ds(pl.multiple_of(i * two, 128), two)

    def attend_loop(qb, kb, vb):
        observed = jnp.sum((mask_ref[...] == 0).astype(jnp.int32), axis=1, keepdims=True)
        row = lax.broadcasted_iota(jnp.int32, (rows, rows), 0)
        column = lax.broadcasted_iota(jnp.int32, (rows, rows), 1)
        allowed = column <= jnp.maximum(row, observed - 1)

        def fetch(i, slot):
            return [
                pltpu.make_async_copy(a.at[:, head_cols(i)], b.at[slot], fetch_sem.at[slot, j])
                for j, (a, b) in enumerate(((q_h, qb), (k_h, kb), (v_h, vb)))
            ]

        def step(i, carry):
            slot = i % 2

            @pl.when(i + 1 < steps)
            def _():
                for copy in fetch(i + 1, 1 - slot):
                    copy.start()

            for copy in fetch(i, slot):
                copy.wait()

            @pl.when(i >= steps - chips)
            def _():
                w_load(1 - t, i - (steps - chips)).start()

            parts = []
            for j in range(2):
                span = slice(j * HEAD_DIM, (j + 1) * HEAD_DIM)
                scores = dot(qb[slot, :, span], kb[slot, :, span], NT) * SCALE
                masked = jnp.where(allowed, scores, -jnp.inf)
                weights = jnp.exp(masked - jnp.max(masked, axis=1, keepdims=True))
                probs = weights * (1.0 / jnp.sum(weights, axis=1, keepdims=True))
                low = probs.astype(jnp.bfloat16)
                probs_v[2 * i + j] = low
                parts.append(jnp.dot(low, vb[slot, :, span], preferred_element_type=jnp.float32))
            att_v[:, head_cols(i)] = jnp.concatenate(parts, axis=1).astype(jnp.bfloat16)
            return carry

        return fetch, step

    def send_half(side):
        gather(att_v, 4, side, z_peer).start()
        gather(att_v, 2, side, x_peer).start()
        gather(att_v, 1, side, core_peer).start()

    def w_load(side, k):
        start = pl.multiple_of(side * width + k * part, part)
        return pltpu.make_async_copy(w_h.at[pl.ds(start, part), :], w_rows(k), w_sem.at[k])

    def w_rows(k):
        return wp.at[pl.ds(pl.multiple_of(k * part, part), part), :]

    def projection(res_v, qb, kb, vb):
        fetch, step = attend_loop(qb, kb, vb)
        for copy in fetch(0, 0):
            copy.start()
        later = [
            pltpu.make_async_copy(a, b, load_sem.at[i + 1])
            for i, (a, b) in enumerate(((res_h, res_v), (ups_h, ups_v), (rg_h, rg_v)))
        ]
        lax.fori_loop(0, steps // 2 + 1, step, 0)
        pl.semaphore_wait(barrier, groups)
        send_half(0)
        lax.fori_loop(steps // 2 + 1, steps, step, 0)

        def give(k, carry):
            w_load(1 - t, k).wait()
            theirs[k] = dot(att_v[...], w_rows(k)[...], NT).astype(jnp.bfloat16)
            remote(theirs.at[k], arrived.at[k], p_sems, (k,), y_peer).start()
            w_load(t, k).start()
            return carry

        lax.fori_loop(0, 1, give, 0)
        send_half(1)
        for copy in later:
            copy.start()
        lax.fori_loop(1, chips, give, 0)
        for copy in later:
            copy.wait()

        def take(k, carry):
            squares, inner = carry
            cols = pl.ds(pl.multiple_of(k * part, 128), part)
            w_load(t, k).wait()
            own = dot(att_v[...], w_rows(k)[...], NT)
            remote(theirs.at[k], arrived.at[k], p_sems, (k,), y_peer).wait()
            total = own + arrived[k].astype(jnp.float32)
            low = (total + res_v[:, cols].astype(jnp.float32)).astype(jnp.bfloat16)
            lo_v[:, cols] = low
            out = low.astype(jnp.float32)
            scaled = ups_v[:, cols].astype(jnp.float32) * gain_ref[:, cols]
            squares = squares + jnp.sum(out * out, axis=1, keepdims=True)
            inner = inner + jnp.sum(scaled * out, axis=1, keepdims=True)
            return squares, inner

        zero = jnp.zeros((rows, 1), jnp.float32)
        carry = lax.fori_loop(0, 2, take, (zero, zero))
        gather(att_v, 4, 0, z_peer).wait_recv()
        gather(gath.at[4], 6, 0, x_peer).start()
        carry = lax.fori_loop(2, 3, take, carry)
        gather(att_v, 2, 1, x_peer).wait_recv()
        gather(gath.at[2], 6, 1, z_peer).start()
        squares, inner = lax.fori_loop(3, chips, take, carry)
        lane = lax.broadcasted_iota(jnp.int32, (rows, 128), 1)
        packed = jnp.where(lane == 0, squares, jnp.where(lane == 1, inner, 0.0))
        sums_mine[...] = jnp.transpose(packed)[0:8]

    pl.run_scoped(
        projection,
        pltpu.VMEM((rows, width), jnp.bfloat16),
        pltpu.VMEM((2, rows, two), jnp.bfloat16),
        pltpu.VMEM((2, rows, two), jnp.bfloat16),
        pltpu.VMEM((2, rows, two), jnp.bfloat16),
    )
    exchange = remote(sums_mine, sums_theirs, s_sems, (0,), y_peer)
    exchange.start()
    lo_out = pltpu.make_async_copy(lo_v, lo_h, load_sem.at[0])
    lo_out.start()
    exchange.wait()
    both = sums_mine[...] + sums_theirs[...]
    wide = jnp.transpose(jnp.concatenate([both, jnp.zeros((120, rows), jnp.float32)], axis=0))
    squares, inner = wide[:, 0:1], wide[:, 1:2]
    rms = jnp.sqrt(squares / model + epsilon)
    inverse = 1.0 / rms
    row_inner = inner / (rms * model)
    slope = row_inner * inverse

    native_kept = 1 - (zh + t) % 2

    def normalise(step_index, carry):
        k = (step_index // 2 * (1 - 2 * t) + t) * 2 + step_index % 2
        cols = pl.ds(pl.multiple_of(k * part, 128), part)
        out = lo_v[:, cols].astype(jnp.float32)
        ups = ups_v[:, cols].astype(jnp.float32)
        scaled = ups * gain_ref[:, cols]
        grad = (rg_v[:, cols].astype(jnp.float32) + (scaled - out * slope) * inverse).astype(jnp.bfloat16)
        gr_v[:, cols] = grad
        turned[k] = jnp.transpose(grad.astype(jnp.float32)).astype(jnp.bfloat16)
        gain_v[d, :, cols] = jnp.sum(ups * (out * inverse), axis=0, keepdims=True)
        remote(turned.at[k], turned_other.at[k], g_sems, (k,), y_peer).start()

        @pl.when(native_kept == 0)
        def _():
            for dc in (0, 1):
                piece(0, turned, k, dc)

        return carry

    lax.fori_loop(0, chips, normalise, 0)
    gr_out = pltpu.make_async_copy(gr_v, gr_h, load_sem.at[1])
    gr_out.start()

    def gain_copy(r, sender):
        return remote(gain_v.at[sender], gain_v.at[sender], gain_sems, (r,), ((d + r) % groups, t))

    for r in range(1, groups):
        gain_copy(r, d).start()
    gather(att_v, 4, 1, z_peer).wait_recv()
    gather(att_v, 2, 0, x_peer).wait_recv()
    for side in (0, 1):
        gather(gath.at[4], 5, side, core_peer).start()
        gather(gath.at[2], 3, side, core_peer).start()

    def cotangent_own(k, carry):
        cols = pl.ds(pl.multiple_of(k * part, 128), part)
        cotangent_sum[:, cols] = jnp.dot(
            gr_v[...], wp[:, cols], preferred_element_type=jnp.float32
        )
        return carry

    lax.fori_loop(0, chips, cotangent_own, 0)
    for k in range(chips):
        w_load(1 - t, k).start()

    def pass_on(step_index, carry):
        k = (1 - t + step_index // 2 * (2 * t - 1)) * 2 + step_index % 2
        remote(turned.at[k], turned_other.at[k], g_sems, (k,), y_peer).wait_recv()
        for dc in (0, 1):
            piece(1, turned_other, k, dc)

        other_v[...] = jnp.transpose(turned_other[k].astype(jnp.float32)).astype(jnp.bfloat16)
        w_load(1 - t, k).wait()

        def add_columns(cb, carry):
            cols = pl.ds(pl.multiple_of(cb * part, 128), part)
            cotangent_sum[:, cols] += jnp.dot(
                other_v[...], w_rows(k)[:, cols], preferred_element_type=jnp.float32
            )
            return carry

        lax.fori_loop(0, chips, add_columns, 0)
        return carry

    lax.fori_loop(0, 1, pass_on, 0)
    for side in (0, 1):
        gather(gath.at[4], 6, side, x_peer).wait_recv()
        gather(gath.at[6], 7, side, core_peer).start()
    lax.fori_loop(1, 2, pass_on, 0)
    for slot in (1, 3, 5, 7):
        for side in (0, 1):
            gather(att_v, slot, side, core_peer).wait_recv()

    blocks = width // part
    far_chip = (zp + 1 - t) % 2

    def finish(kept, att_b):
        def block_load(cb, slot):
            cols = pl.ds(pl.multiple_of(cb * part, 128), part)
            copies = [
                pltpu.make_async_copy(
                    att_v.at[:, cols], att_b.at[slot, 0:rows, :], block_sem.at[slot, 0]
                )
            ]
            for delta in range(1, 8):
                copies.append(
                    pltpu.make_async_copy(
                        gath.at[delta, :, cols],
                        att_b.at[slot, delta * rows : (delta + 1) * rows, :],
                        block_sem.at[slot, delta],
                    )
                )
            return copies

        def mid_copy(cb):
            return remote(mid_out.at[cb], mid_in.at[cb], mid_sems, (cb,), mid_peer)

        def kept_copy(cb):
            cols = pl.ds(pl.multiple_of(cb * part, 128), part)
            return pltpu.make_async_copy(kept.at[cb], kept_h.at[:, cols], final_sem.at[cb])

        def multiply(kind):
            for copy in block_load(0, 0):
                copy.start()
            for delta in range(8):
                pltpu.make_async_copy(
                    turned.at[0, 0:own_rows, :],
                    pieces.at[kind, :, delta * rows : (delta + 1) * rows],
                    piece_sems.at[1, kind, delta],
                ).wait()
            keeps = (kind + native_kept) % 2 == 1

            def product(cb, carry):
                slot = cb % 2

                @pl.when(cb + 1 < blocks)
                def _():
                    for copy in block_load(cb + 1, 1 - slot):
                        copy.start()

                for copy in block_load(cb, slot):
                    copy.wait()
                value = jnp.dot(pieces[kind], att_b[slot], preferred_element_type=jnp.float32)

                @pl.when(keeps)
                def _():
                    kept[cb] = value
                    kept_copy(cb).start()

                @pl.when(jnp.logical_not(keeps))
                def _():
                    mid_out[cb] = value.astype(jnp.bfloat16)
                    mid_copy(cb).start()

                return carry

            lax.fori_loop(0, blocks, product, 0)

        @pl.when(native_kept == 0)
        def _():
            multiply(0)

        lax.fori_loop(2, chips, pass_on, 0)

        @pl.when(native_kept == 1)
        def _():
            for k in range(chips):
                for dc in (0, 1):
                    piece(0, turned, k, dc)

        def attention(qb, kb, vb, ob):
            def fetch(i, slot):
                cols = pl.ds(pl.multiple_of(i * 2 * HEAD_DIM, 128), 2 * HEAD_DIM)
                pairs = (
                    (q_h.at[:, cols], qb),
                    (k_h.at[:, cols], kb),
                    (v_h.at[:, cols], vb),
                )
                return [
                    pltpu.make_async_copy(a, b.at[slot], fetch_sem.at[slot, j])
                    for j, (a, b) in enumerate(pairs)
                ]

            def emit(i, slot):
                cols = pl.ds(pl.multiple_of(i * 2 * HEAD_DIM, 128), 2 * HEAD_DIM)
                return [
                    pltpu.make_async_copy(ob.at[slot, j], b.at[:, cols], out_sem.at[slot, j])
                    for j, b in enumerate((gq_h, gk_h, gv_h))
                ]

            for copy in fetch(0, 0):
                copy.start()

            def step(i, carry):
                slot = i % 2

                @pl.when(i + 1 < steps)
                def _():
                    for copy in fetch(i + 1, 1 - slot):
                        copy.start()

                for copy in fetch(i, slot):
                    copy.wait()

                @pl.when(i >= 2)
                def _():
                    for copy in emit(i - 2, slot):
                        copy.wait()

                cotangents = cotangent_sum[:, head_cols(i)].astype(jnp.bfloat16)
                for j in range(2):
                    span = slice(j * HEAD_DIM, (j + 1) * HEAD_DIM)
                    low = probs_v[2 * i + j]
                    cotangent = cotangents[:, span]
                    ob[slot, 2, :, span] = dot(low, cotangent, TN).astype(jnp.bfloat16)
                    grad_probs = dot(cotangent, vb[slot, :, span], NT)
                    probs = low.astype(jnp.float32)
                    delta = jnp.sum(probs * grad_probs, axis=1, keepdims=True)
                    grad_scores = (probs * (grad_probs - delta) * SCALE).astype(jnp.bfloat16)
                    ob[slot, 0, :, span] = jnp.dot(
                        grad_scores, kb[slot, :, span], preferred_element_type=jnp.float32
                    ).astype(jnp.bfloat16)
                    ob[slot, 1, :, span] = dot(grad_scores, qb[slot, :, span], TN).astype(
                        jnp.bfloat16
                    )
                for copy in emit(i, slot):
                    copy.start()
                return carry

            early = 2 * far_chip
            lax.fori_loop(0, early, step, 0)

            @pl.when(native_kept == 1)
            def _():
                multiply(1)

            lax.fori_loop(early, steps, step, 0)
            multiply(1 - native_kept)
            for i in (steps - 2, steps - 1):
                for copy in emit(i, i % 2):
                    copy.wait()

        pl.run_scoped(
            attention,
            pltpu.VMEM((2, rows, two), jnp.bfloat16),
            pltpu.VMEM((2, rows, two), jnp.bfloat16),
            pltpu.VMEM((2, rows, two), jnp.bfloat16),
            pltpu.VMEM((2, 3, rows, two), jnp.bfloat16),
        )
        for r in range(1, groups):
            gain_copy(r, (d + groups - r) % groups).wait()
        total = gain_v[0]
        for i in range(1, groups):
            total = total + gain_v[i]
        gain_o[...] = jnp.reshape(total, (width,))

        for cb in range(blocks):
            mid_copy(cb).wait()
            kept_copy(cb).wait()

    pl.run_scoped(
        finish,
        pltpu.VMEM((blocks, own_rows, part), jnp.float32),
        pltpu.VMEM((2, 8 * rows, part), jnp.bfloat16),
    )
    lo_out.wait()
    gr_out.wait()
    for k in range(chips):
        remote(turned.at[k], turned_other.at[k], g_sems, (k,), y_peer).wait_send()
    for slot in range(1, 8):
        for side in (0, 1):
            gather(att_v, slot, side, core_peer).wait_send()
    for kind in (0, 1):
        for delta in range(1, 8):
            remote(
                turned.at[0, 0:own_rows, :],
                pieces.at[kind, :, 0:rows],
                piece_sems,
                (kind, delta),
                core_peer,
            ).wait_send()


def trunk(groups, mask, gain, res, ups, rg, weight, q, k, v):
    rows, width = q.shape
    model = weight.shape[0]
    chips = 4
    part = width // chips
    own_rows = part // 2
    two = 2 * HEAD_DIM
    anywhere = pl.BlockSpec(memory_space=pl.ANY)
    local = pl.BlockSpec(memory_space=pltpu.VMEM)
    low = jnp.bfloat16
    act = jax.ShapeDtypeStruct((rows, width), low)
    dma = pltpu.SemaphoreType.DMA
    return pl.pallas_call(
        functools.partial(trunk_kernel, groups),
        in_specs=[local] * 2 + [anywhere] * 7,
        out_specs=[anywhere] * 7 + [local, anywhere],
        out_shape=[act] * 5
        + [
            jax.ShapeDtypeStruct((own_rows, width), jnp.float32),
            jax.ShapeDtypeStruct((chips, own_rows, part), low),
            jax.ShapeDtypeStruct((width,), jnp.float32),
            jax.ShapeDtypeStruct((8, rows, width), low),
        ],
        scratch_shapes=[
            pltpu.VMEM((rows, width), low),
            pltpu.VMEM((width // HEAD_DIM, rows, rows), low),
            pltpu.VMEM((rows, width), low),
            pltpu.VMEM((rows, width), low),
            pltpu.VMEM((1, width), jnp.float32),
            pltpu.VMEM((chips, rows, part), low),
            pltpu.VMEM((chips, rows, part), low),
            pltpu.VMEM((rows, width), low),
            pltpu.VMEM((rows, width), low),
            pltpu.VMEM((chips, part, rows), low),
            pltpu.VMEM((chips, part, rows), low),
            pltpu.VMEM((rows, part), low),
            pltpu.VMEM((width, width), low),
            pltpu.VMEM((rows, width), jnp.float32),
            pltpu.VMEM((2, own_rows, 8 * rows), low),
            pltpu.VMEM((8, rows), jnp.float32),
            pltpu.VMEM((8, rows), jnp.float32),
            pltpu.VMEM((groups, 1, width), jnp.float32),
            pltpu.VMEM((chips, own_rows, part), low),
            dma((4,)),
            dma((chips,)),
            dma((2, chips)),
            dma((2, chips)),
            dma((2, 1)),
            dma((2, 8, 2)),
            dma((2, 2, 8)),
            dma((2, groups)),
            dma((2, chips)),
            dma((2, 8)),
            dma((2, 4)),
            dma((2, 3)),
            dma((chips,)),
        ],
        compiler_params=pltpu.CompilerParams(
            collective_id=0, has_side_effects=True, vmem_limit_bytes=66 * 1000 * 1000
        ),
        name="trunk",
    )(mask, gain, res, ups, rg, weight, q, k, v)


def hand_out_kernel(*refs):
    for a, b in zip(refs[:5], refs[7:12]):
        b[...] = a[...]
    refs[12][...] = refs[5][...] + refs[6][...].astype(jnp.float32)


def hand_out(arrays, kept, arrived):
    rows, width = arrays[0].shape
    own_rows = kept.shape[0]
    steps, part = arrived.shape[0], arrived.shape[2]
    act = pl.BlockSpec((rows // steps, width), lambda i: (i, 0))
    column = pl.BlockSpec((own_rows, part), lambda i: (0, i))
    return pl.pallas_call(
        hand_out_kernel,
        grid=(steps,),
        in_specs=[act] * 5 + [column, pl.BlockSpec((None, own_rows, part), lambda i: (i, 0, 0))],
        out_specs=[act] * 5 + [column],
        out_shape=[jax.ShapeDtypeStruct((rows, width), jnp.bfloat16)] * 5
        + [jax.ShapeDtypeStruct((own_rows, width), jnp.float32)],
        name="hand_out",
    )(*arrays, kept, arrived)


def sum_groups(groups, value):
    if groups & (groups - 1):
        return lax.psum(value, "dp")
    bit = 1
    while bit < groups:
        value = value + lax.ppermute(value, "dp", [(i, i ^ bit) for i in range(groups)])
        bit *= 2
    return value


def shards(
    groups,
    tensor_size,
    query_rows,
    key_rows,
    value_rows,
    action_mask,
    residual,
    out_weight,
    norm_gain,
    upstream,
    residual_grad,
):
    model_width = out_weight.shape[0]
    own_width = residual.shape[1]
    pair = tensor_size == 2
    swap = [(0, 1), (1, 0)]
    mine = lax.axis_index("tensor")

    def weight_rows(index):
        return lax.dynamic_slice_in_dim(out_weight, index * own_width, own_width, 0)

    def sum_pair(value):
        if pair:
            return value + lax.ppermute(value, "tensor", swap)
        return lax.psum(value, "tensor")

    if pair and groups == 16 and query_rows.shape[0] == LEN:
        out = trunk(
            groups,
            action_mask,
            norm_gain,
            residual,
            upstream,
            residual_grad,
            out_weight,
            query_rows,
            key_rows,
            value_rows,
        )
        return (*hand_out(out[:5], out[5], out[6]), out[7])
    observed = jnp.sum((action_mask == 0).astype(jnp.int32), axis=1)
    probs, attended = attend(observed, query_rows, key_rows, value_rows)
    attended_all = lax.all_gather(attended, "dp", axis=0, tiled=True)
    if pair:
        theirs = dot(attended, weight_rows(1 - mine), NT).astype(jnp.bfloat16)
        arriving = lax.ppermute(theirs, "tensor", swap)
        own = dot(attended, weight_rows(mine), NT)
        own_sum = own + arriving.astype(jnp.float32)
    else:
        own_sum = lax.psum_scatter(
            dot(attended, out_weight, NT), "tensor", scatter_dimension=1, tiled=True
        )
    layer_out = (own_sum + residual.astype(jnp.float32)).astype(jnp.bfloat16)
    out_float = layer_out.astype(jnp.float32)
    upstream_float = upstream.astype(jnp.float32)
    scaled = upstream_float * norm_gain[None, :]
    sums = sum_pair(
        jnp.stack([jnp.sum(out_float * out_float, axis=1), jnp.sum(scaled * out_float, axis=1)])
    )
    row_rms = jnp.sqrt(sums[0] / model_width + epsilon)[:, None]
    normed = out_float / row_rms
    row_inner = sums[1][:, None] / (row_rms * model_width)
    grad_residual = (
        residual_grad.astype(jnp.float32) + (scaled - normed * row_inner) / row_rms
    ).astype(jnp.bfloat16)
    if pair:
        other = lax.ppermute(grad_residual, "tensor", swap)
        first = mine == 0
        low_half = jnp.where(first, grad_residual, other)
        high_half = jnp.where(first, other, grad_residual)
        grad_full = jnp.concatenate([low_half, high_half], axis=1)
        grad_attended = jnp.dot(
            grad_residual, weight_rows(mine), preferred_element_type=jnp.float32
        ) + jnp.dot(other, weight_rows(1 - mine), preferred_element_type=jnp.float32)
    else:
        grad_full = lax.all_gather(grad_residual, "tensor", axis=1, tiled=True)
        grad_attended = jnp.dot(grad_full, out_weight, preferred_element_type=jnp.float32)
    grad_attended = grad_attended.astype(jnp.bfloat16)
    received = lax.all_to_all(grad_full, "dp", split_axis=1, concat_axis=0, tiled=True)
    gain_part = jnp.sum(upstream_float * normed, axis=0)
    grad_query, grad_key, grad_value = attend_backward(
        probs, query_rows, key_rows, value_rows, grad_attended
    )
    grad_query, gain_part = lax.optimization_barrier((grad_query, gain_part))
    grad_gain = sum_groups(groups, gain_part)
    grad_out_weight = dot(received, attended_all, TN)
    return layer_out, grad_residual, grad_query, grad_key, grad_value, grad_out_weight, grad_gain


def solution(mesh):
    rows = P("dp", "tensor")
    return jax.shard_map(
        functools.partial(shards, mesh.shape["dp"], mesh.shape["tensor"]),
        mesh=mesh,
        in_specs=(
            rows,
            rows,
            rows,
            P("dp", None),
            rows,
            P(None, "tensor"),
            P("tensor"),
            rows,
            rows,
        ),
        out_specs=(rows, rows, rows, rows, rows, rows, P("tensor")),
        check_vma=False,
    )
```

```python
import functools

import jax
import jax.numpy as jnp
from jax import lax
from jax.experimental import pallas as pl
from jax.experimental.pallas import tpu as pltpu
from jax.sharding import PartitionSpec as P

HEAD_DIM = 128
LEN = 384

epsilon = 1e-05
SCALE = HEAD_DIM ** (-0.5)
NT = (((1,), (1,)), ((), ()))
TN = (((0,), (0,)), ((), ()))


def dot(a, b, dims):
    return lax.dot_general(a, b, dims, preferred_element_type=jnp.float32)


def forward_kernel(heads, observed_ref, query_ref, key_ref, value_ref, probs_ref, attended_ref):
    observed = observed_ref[pl.program_id(0)]
    row = lax.broadcasted_iota(jnp.int32, (LEN, LEN), 0)
    column = lax.broadcasted_iota(jnp.int32, (LEN, LEN), 1)
    allowed = column <= jnp.maximum(row, observed - 1)
    for head in range(heads):
        span = slice(head * HEAD_DIM, (head + 1) * HEAD_DIM)
        scores = dot(query_ref[:, span], key_ref[:, span], NT) * SCALE
        masked = jnp.where(allowed, scores, -jnp.inf)
        weights = jnp.exp(masked - jnp.max(masked, axis=1, keepdims=True))
        probs = weights * (1.0 / jnp.sum(weights, axis=1, keepdims=True))
        low = probs.astype(jnp.bfloat16)
        probs_ref[head] = low
        attended_ref[:, span] = jnp.dot(
            low, value_ref[:, span], preferred_element_type=jnp.float32
        ).astype(jnp.bfloat16)


def backward_kernel(
    heads, probs_ref, query_ref, key_ref, value_ref, cotangent_ref, query_out, key_out, value_out
):
    for head in range(heads):
        span = slice(head * HEAD_DIM, (head + 1) * HEAD_DIM)
        low = probs_ref[head]
        cotangent = cotangent_ref[:, span]
        value_out[:, span] = dot(low, cotangent, TN).astype(jnp.bfloat16)
        grad_probs = dot(cotangent, value_ref[:, span], NT)
        probs = low.astype(jnp.float32)
        delta = jnp.sum(probs * grad_probs, axis=1, keepdims=True)
        grad_scores = (probs * (grad_probs - delta) * SCALE).astype(jnp.bfloat16)
        query_out[:, span] = jnp.dot(
            grad_scores, key_ref[:, span], preferred_element_type=jnp.float32
        ).astype(jnp.bfloat16)
        key_out[:, span] = dot(grad_scores, query_ref[:, span], TN).astype(jnp.bfloat16)


def head_group(head_count):
    return max(size for size in range(1, 6) if head_count % size == 0)


def specs(heads):
    rows = pl.BlockSpec((LEN, heads * HEAD_DIM), lambda s, h: (s, h))
    square = pl.BlockSpec((None, heads, LEN, LEN), lambda s, h: (s, h, 0, 0))
    return rows, square


def attend(observed, query_rows, key_rows, value_rows):
    tok_rows, width = query_rows.shape
    head_count, seq_count = width // HEAD_DIM, tok_rows // LEN
    heads = head_group(head_count)
    rows, square = specs(heads)
    pairs = seq_count * head_count * LEN * LEN
    return pl.pallas_call(
        functools.partial(forward_kernel, heads),
        grid=(seq_count, head_count // heads),
        in_specs=[pl.BlockSpec(memory_space=pltpu.SMEM), rows, rows, rows],
        out_specs=[square, rows],
        out_shape=[
            jax.ShapeDtypeStruct((seq_count, head_count, LEN, LEN), jnp.bfloat16),
            jax.ShapeDtypeStruct((tok_rows, width), jnp.bfloat16),
        ],
        cost_estimate=pl.CostEstimate(
            flops=4 * pairs * HEAD_DIM,
            bytes_accessed=2 * pairs + 8 * tok_rows * width,
            transcendentals=pairs,
        ),
        name="attend",
    )(observed, query_rows, key_rows, value_rows)


def attend_backward(probs, query_rows, key_rows, value_rows, cotangent):
    tok_rows, width = query_rows.shape
    head_count, seq_count = width // HEAD_DIM, tok_rows // LEN
    heads = head_group(head_count)
    rows, square = specs(heads)
    pairs = seq_count * head_count * LEN * LEN
    return pl.pallas_call(
        functools.partial(backward_kernel, heads),
        grid=(seq_count, head_count // heads),
        in_specs=[square, rows, rows, rows, rows],
        out_specs=[rows, rows, rows],
        out_shape=[jax.ShapeDtypeStruct((tok_rows, width), jnp.bfloat16)] * 3,
        cost_estimate=pl.CostEstimate(
            flops=8 * pairs * HEAD_DIM,
            bytes_accessed=2 * pairs + 14 * tok_rows * width,
            transcendentals=0,
        ),
        name="attend_backward",
    )(probs, query_rows, key_rows, value_rows, cotangent)


MESH = pl.DeviceIdType.MESH


def trunk_kernel(
    groups,
    mask_ref,
    gain_h,
    res_h,
    ups_h,
    rg_h,
    w_h,
    q_h,
    k_h,
    v_h,
    lo_h,
    gr_h,
    gq_h,
    gk_h,
    gv_h,
    kept_h,
    mid_in,
    gain_o,
    gath,
    att_v,
    probs_v,
    ups_v,
    rg_v,
    gain_ref,
    theirs,
    arrived,
    lo_v,
    gr_v,
    turned,
    turned_other,
    other_v,
    wp,
    cotangent_sum,
    pieces,
    sums_mine,
    sums_theirs,
    gain_v,
    mid_out,
    load_sem,
    w_sem,
    p_sems,
    g_sems,
    s_sems,
    ag_sems,
    piece_sems,
    gain_sems,
    mid_sems,
    block_sem,
    fetch_sem,
    out_sem,
    final_sem,
):
    rows, width = att_v.shape
    model = 2 * width
    chips = 4
    part = width // chips
    own_rows = part // 2
    half = width // 2
    d = lax.axis_index("dp")
    t = lax.axis_index("tensor")
    c = d % 2
    x = (d // 2) % 2
    zp = (d // 4) % 2
    zh = d // 8

    def device(zh_, zp_, x_, c_, t_):
        return (((zh_ * 2 + zp_) * 2 + x_) * 2 + c_, t_)

    y_peer = (d, 1 - t)
    x_peer = device(zh, zp, 1 - x, c, t)
    z_peer = device(zh, 1 - zp, x, c, t)
    core_peer = device(zh, zp, x, 1 - c, t)
    mid_peer = device(1 - zh, zp, x, c, t)

    def remote(src, dst, sems, index, target):
        return pltpu.make_async_remote_copy(
            src_ref=src,
            dst_ref=dst,
            send_sem=sems.at[(0,) + index],
            recv_sem=sems.at[(1,) + index],
            device_id=target,
            device_id_type=MESH,
        )

    barrier = pltpu.get_barrier_semaphore()
    for r in range(1, groups):
        pl.semaphore_signal(barrier, inc=1, device_id=((d + r) % groups, t), device_id_type=MESH)
    pl.semaphore_signal(barrier, inc=1, device_id=y_peer, device_id_type=MESH)

    def gather(src, slot, side, target):
        cols = slice(side * half, (side + 1) * half)
        return remote(src.at[:, cols], gath.at[slot, :, cols], ag_sems, (slot, side), target)

    def piece(kind, source, k, dc):
        kz, kx = k // 2, k % 2
        dz = zp + kz - 2 * zp * kz
        dx = x + kx - 2 * x * kx
        core = c + dc - 2 * c * dc
        delta = dz * 4 + dx * 2 + dc
        src = source.at[k, pl.ds(core * own_rows, own_rows), :]
        dst = pieces.at[kind, :, pl.ds(pl.multiple_of(delta * rows, 128), rows)]
        far = remote(src, dst, piece_sems, (kind, delta), device(zh, kz, kx, core, t))
        if dc == 1:
            far.start()
        else:

            @pl.when(dz + dx > 0)
            def _():
                far.start()

            @pl.when(dz + dx == 0)
            def _():
                pltpu.make_async_copy(src, pieces.at[kind, :, 0:rows], piece_sems.at[1, kind, 0]).start()

    gain_ref[...] = jnp.reshape(gain_h[...], (1, width))
    two = 2 * HEAD_DIM
    steps = width // two

    def head_cols(i):
        return pl.ds(pl.multiple_of(i * two, 128), two)

    def attend_loop(qb, kb, vb):
        observed = jnp.sum((mask_ref[...] == 0).astype(jnp.int32), axis=1, keepdims=True)
        row = lax.broadcasted_iota(jnp.int32, (rows, rows), 0)
        column = lax.broadcasted_iota(jnp.int32, (rows, rows), 1)
        allowed = column <= jnp.maximum(row, observed - 1)

        def fetch(i, slot):
            return [
                pltpu.make_async_copy(a.at[:, head_cols(i)], b.at[slot], fetch_sem.at[slot, j])
                for j, (a, b) in enumerate(((q_h, qb), (k_h, kb), (v_h, vb)))
            ]

        def step(i, carry):
            slot = i % 2

            @pl.when(i + 1 < steps)
            def _():
                for copy in fetch(i + 1, 1 - slot):
                    copy.start()

            for copy in fetch(i, slot):
                copy.wait()

            @pl.when(i >= steps - chips)
            def _():
                w_load(1 - t, i - (steps - chips)).start()

            parts = []
            for j in range(2):
                span = slice(j * HEAD_DIM, (j + 1) * HEAD_DIM)
                scores = dot(qb[slot, :, span], kb[slot, :, span], NT) * SCALE
                masked = jnp.where(allowed, scores, -jnp.inf)
                weights = jnp.exp(masked - jnp.max(masked, axis=1, keepdims=True))
                probs = weights * (1.0 / jnp.sum(weights, axis=1, keepdims=True))
                low = probs.astype(jnp.bfloat16)
                probs_v[2 * i + j] = low
                parts.append(jnp.dot(low, vb[slot, :, span], preferred_element_type=jnp.float32))
            att_v[:, head_cols(i)] = jnp.concatenate(parts, axis=1).astype(jnp.bfloat16)
            return carry

        return fetch, step

    def send_half(side):
        gather(att_v, 4, side, z_peer).start()
        gather(att_v, 2, side, x_peer).start()
        gather(att_v, 1, side, core_peer).start()

    def w_load(side, k):
        start = pl.multiple_of(side * width + k * part, part)
        return pltpu.make_async_copy(w_h.at[pl.ds(start, part), :], w_rows(k), w_sem.at[k])

    def w_rows(k):
        return wp.at[pl.ds(pl.multiple_of(k * part, part), part), :]

    def projection(res_v, qb, kb, vb):
        fetch, step = attend_loop(qb, kb, vb)
        for copy in fetch(0, 0):
            copy.start()
        later = [
            pltpu.make_async_copy(a, b, load_sem.at[i + 1])
            for i, (a, b) in enumerate(((res_h, res_v), (ups_h, ups_v), (rg_h, rg_v)))
        ]
        lax.fori_loop(0, steps // 2 + 1, step, 0)
        pl.semaphore_wait(barrier, groups)
        send_half(0)
        lax.fori_loop(steps // 2 + 1, steps, step, 0)

        def give(k, carry):
            w_load(1 - t, k).wait()
            theirs[k] = dot(att_v[...], w_rows(k)[...], NT).astype(jnp.bfloat16)
            remote(theirs.at[k], arrived.at[k], p_sems, (k,), y_peer).start()
            w_load(t, k).start()
            return carry

        lax.fori_loop(0, 1, give, 0)
        send_half(1)
        for copy in later:
            copy.start()
        lax.fori_loop(1, chips, give, 0)
        for copy in later:
            copy.wait()

        def take(k, carry):
            squares, inner = carry
            cols = pl.ds(pl.multiple_of(k * part, 128), part)
            w_load(t, k).wait()
            own = dot(att_v[...], w_rows(k)[...], NT)
            remote(theirs.at[k], arrived.at[k], p_sems, (k,), y_peer).wait()
            total = own + arrived[k].astype(jnp.float32)
            low = (total + res_v[:, cols].astype(jnp.float32)).astype(jnp.bfloat16)
            lo_v[:, cols] = low
            out = low.astype(jnp.float32)
            scaled = ups_v[:, cols].astype(jnp.float32) * gain_ref[:, cols]
            squares = squares + jnp.sum(out * out, axis=1, keepdims=True)
            inner = inner + jnp.sum(scaled * out, axis=1, keepdims=True)
            return squares, inner

        zero = jnp.zeros((rows, 1), jnp.float32)
        carry = lax.fori_loop(0, 2, take, (zero, zero))
        gather(att_v, 4, 0, z_peer).wait_recv()
        gather(gath.at[4], 6, 0, x_peer).start()
        carry = lax.fori_loop(2, 3, take, carry)
        gather(att_v, 2, 1, x_peer).wait_recv()
        gather(gath.at[2], 6, 1, z_peer).start()
        squares, inner = lax.fori_loop(3, chips, take, carry)
        lane = lax.broadcasted_iota(jnp.int32, (rows, 128), 1)
        packed = jnp.where(lane == 0, squares, jnp.where(lane == 1, inner, 0.0))
        sums_mine[...] = jnp.transpose(packed)[0:8]

    pl.run_scoped(
        projection,
        pltpu.VMEM((rows, width), jnp.bfloat16),
        pltpu.VMEM((2, rows, two), jnp.bfloat16),
        pltpu.VMEM((2, rows, two), jnp.bfloat16),
        pltpu.VMEM((2, rows, two), jnp.bfloat16),
    )
    exchange = remote(sums_mine, sums_theirs, s_sems, (0,), y_peer)
    exchange.start()
    lo_out = pltpu.make_async_copy(lo_v, lo_h, load_sem.at[0])
    lo_out.start()
    exchange.wait()
    both = sums_mine[...] + sums_theirs[...]
    wide = jnp.transpose(jnp.concatenate([both, jnp.zeros((120, rows), jnp.float32)], axis=0))
    squares, inner = wide[:, 0:1], wide[:, 1:2]
    rms = jnp.sqrt(squares / model + epsilon)
    inverse = 1.0 / rms
    row_inner = inner / (rms * model)
    slope = row_inner * inverse

    native_kept = 1 - (zh + t) % 2

    def normalise(step_index, carry):
        k = (step_index // 2 * (1 - 2 * t) + t) * 2 + step_index % 2
        cols = pl.ds(pl.multiple_of(k * part, 128), part)
        out = lo_v[:, cols].astype(jnp.float32)
        ups = ups_v[:, cols].astype(jnp.float32)
        scaled = ups * gain_ref[:, cols]
        grad = (rg_v[:, cols].astype(jnp.float32) + (scaled - out * slope) * inverse).astype(jnp.bfloat16)
        gr_v[:, cols] = grad
        turned[k] = jnp.transpose(grad.astype(jnp.float32)).astype(jnp.bfloat16)
        gain_v[d, :, cols] = jnp.sum(ups * (out * inverse), axis=0, keepdims=True)
        remote(turned.at[k], turned_other.at[k], g_sems, (k,), y_peer).start()

        @pl.when(native_kept * (step_index // 2) == 0)
        def _():
            for dc in (0, 1):
                piece(0, turned, k, dc)

        return carry

    lax.fori_loop(0, chips, normalise, 0)
    gr_out = pltpu.make_async_copy(gr_v, gr_h, load_sem.at[1])
    gr_out.start()

    def gain_copy(r, sender):
        return remote(gain_v.at[sender], gain_v.at[sender], gain_sems, (r,), ((d + r) % groups, t))

    for r in range(1, groups):
        gain_copy(r, d).start()
    gather(att_v, 4, 1, z_peer).wait_recv()
    gather(att_v, 2, 0, x_peer).wait_recv()
    for side in (0, 1):
        gather(gath.at[4], 5, side, core_peer).start()
        gather(gath.at[2], 3, side, core_peer).start()

    def cotangent_own(k, carry):
        cols = pl.ds(pl.multiple_of(k * part, 128), part)
        cotangent_sum[:, cols] = jnp.dot(
            gr_v[...], wp[:, cols], preferred_element_type=jnp.float32
        )
        return carry

    lax.fori_loop(0, chips, cotangent_own, 0)
    for k in range(chips):
        w_load(1 - t, k).start()

    def arrival(step_index):
        return (1 - t + step_index // 2 * (2 * t - 1)) * 2 + step_index % 2

    def pass_on(step_index, carry):
        k = arrival(step_index)
        remote(turned.at[k], turned_other.at[k], g_sems, (k,), y_peer).wait_recv()

        @pl.when(native_kept + step_index // 2 > 0)
        def _():
            for dc in (0, 1):
                piece(1, turned_other, k, dc)


        other_v[...] = jnp.transpose(turned_other[k].astype(jnp.float32)).astype(jnp.bfloat16)
        w_load(1 - t, k).wait()

        def add_columns(cb, carry):
            cols = pl.ds(pl.multiple_of(cb * part, 128), part)
            cotangent_sum[:, cols] += jnp.dot(
                other_v[...], w_rows(k)[:, cols], preferred_element_type=jnp.float32
            )
            return carry

        lax.fori_loop(0, chips, add_columns, 0)
        return carry

    lax.fori_loop(0, 1, pass_on, 0)
    for side in (0, 1):
        gather(gath.at[4], 6, side, x_peer).wait_recv()
        gather(gath.at[6], 7, side, core_peer).start()
    lax.fori_loop(1, 2, pass_on, 0)
    for slot in (1, 3, 5, 7):
        for side in (0, 1):
            gather(att_v, slot, side, core_peer).wait_recv()

    blocks = width // part
    far_chip = (zp + 1 - t) % 2

    def finish(kept, att_b):
        def block_load(cb, slot):
            cols = pl.ds(pl.multiple_of(cb * part, 128), part)
            copies = [
                pltpu.make_async_copy(
                    att_v.at[:, cols], att_b.at[slot, 0:rows, :], block_sem.at[slot, 0]
                )
            ]
            for delta in range(1, 8):
                copies.append(
                    pltpu.make_async_copy(
                        gath.at[delta, :, cols],
                        att_b.at[slot, delta * rows : (delta + 1) * rows, :],
                        block_sem.at[slot, delta],
                    )
                )
            return copies

        def mid_copy(cb):
            return remote(mid_out.at[cb], mid_in.at[cb], mid_sems, (cb,), mid_peer)

        def kept_copy(cb):
            cols = pl.ds(pl.multiple_of(cb * part, 128), part)
            return pltpu.make_async_copy(kept.at[cb], kept_h.at[:, cols], final_sem.at[cb])

        def multiply(kind):
            for copy in block_load(0, 0):
                copy.start()
            for delta in range(8):
                pltpu.make_async_copy(
                    turned.at[0, 0:own_rows, :],
                    pieces.at[kind, :, delta * rows : (delta + 1) * rows],
                    piece_sems.at[1, kind, delta],
                ).wait()
            keeps = (kind + native_kept) % 2 == 1

            def product(cb, carry):
                slot = cb % 2

                @pl.when(cb + 1 < blocks)
                def _():
                    for copy in block_load(cb + 1, 1 - slot):
                        copy.start()

                for copy in block_load(cb, slot):
                    copy.wait()
                value = jnp.dot(pieces[kind], att_b[slot], preferred_element_type=jnp.float32)

                @pl.when(keeps)
                def _():
                    kept[cb] = value
                    kept_copy(cb).start()

                @pl.when(jnp.logical_not(keeps))
                def _():
                    mid_out[cb] = value.astype(jnp.bfloat16)
                    mid_copy(cb).start()

                return carry

            lax.fori_loop(0, blocks, product, 0)

        @pl.when(native_kept == 0)
        def _():
            multiply(0)
            for i in (0, 1):
                for dc in (0, 1):
                    piece(1, turned_other, arrival(i), dc)

        lax.fori_loop(2, 3, pass_on, 0)

        @pl.when(native_kept * (1 - far_chip) == 1)
        def _():
            multiply(1)

        lax.fori_loop(3, chips, pass_on, 0)

        @pl.when(native_kept == 1)
        def _():
            for i in (0, 1):
                for dc in (0, 1):
                    piece(0, turned, arrival(i), dc)

        def attention(qb, kb, vb, ob):
            def fetch(i, slot):
                cols = pl.ds(pl.multiple_of(i * 2 * HEAD_DIM, 128), 2 * HEAD_DIM)
                pairs = (
                    (q_h.at[:, cols], qb),
                    (k_h.at[:, cols], kb),
                    (v_h.at[:, cols], vb),
                )
                return [
                    pltpu.make_async_copy(a, b.at[slot], fetch_sem.at[slot, j])
                    for j, (a, b) in enumerate(pairs)
                ]

            def emit(i, slot):
                cols = pl.ds(pl.multiple_of(i * 2 * HEAD_DIM, 128), 2 * HEAD_DIM)
                return [
                    pltpu.make_async_copy(ob.at[slot, j], b.at[:, cols], out_sem.at[slot, j])
                    for j, b in enumerate((gq_h, gk_h, gv_h))
                ]

            for copy in fetch(0, 0):
                copy.start()

            def step(i, carry):
                slot = i % 2

                @pl.when(i + 1 < steps)
                def _():
                    for copy in fetch(i + 1, 1 - slot):
                        copy.start()

                for copy in fetch(i, slot):
                    copy.wait()

                @pl.when(i >= 2)
                def _():
                    for copy in emit(i - 2, slot):
                        copy.wait()

                cotangents = cotangent_sum[:, head_cols(i)].astype(jnp.bfloat16)
                for j in range(2):
                    span = slice(j * HEAD_DIM, (j + 1) * HEAD_DIM)
                    low = probs_v[2 * i + j]
                    cotangent = cotangents[:, span]
                    ob[slot, 2, :, span] = dot(low, cotangent, TN).astype(jnp.bfloat16)
                    grad_probs = dot(cotangent, vb[slot, :, span], NT)
                    probs = low.astype(jnp.float32)
                    delta = jnp.sum(probs * grad_probs, axis=1, keepdims=True)
                    grad_scores = (probs * (grad_probs - delta) * SCALE).astype(jnp.bfloat16)
                    ob[slot, 0, :, span] = jnp.dot(
                        grad_scores, kb[slot, :, span], preferred_element_type=jnp.float32
                    ).astype(jnp.bfloat16)
                    ob[slot, 1, :, span] = dot(grad_scores, qb[slot, :, span], TN).astype(
                        jnp.bfloat16
                    )
                for copy in emit(i, slot):
                    copy.start()
                return carry

            early = 2 * far_chip
            lax.fori_loop(0, early, step, 0)

            @pl.when(native_kept * far_chip == 1)
            def _():
                multiply(1)

            lax.fori_loop(early, steps, step, 0)
            multiply(1 - native_kept)
            for i in (steps - 2, steps - 1):
                for copy in emit(i, i % 2):
                    copy.wait()

        pl.run_scoped(
            attention,
            pltpu.VMEM((2, rows, two), jnp.bfloat16),
            pltpu.VMEM((2, rows, two), jnp.bfloat16),
            pltpu.VMEM((2, rows, two), jnp.bfloat16),
            pltpu.VMEM((2, 3, rows, two), jnp.bfloat16),
        )
        for r in range(1, groups):
            gain_copy(r, (d + groups - r) % groups).wait()
        total = gain_v[0]
        for i in range(1, groups):
            total = total + gain_v[i]
        gain_o[...] = jnp.reshape(total, (width,))

        for cb in range(blocks):
            mid_copy(cb).wait()
            kept_copy(cb).wait()

    pl.run_scoped(
        finish,
        pltpu.VMEM((blocks, own_rows, part), jnp.float32),
        pltpu.VMEM((2, 8 * rows, part), jnp.bfloat16),
    )
    lo_out.wait()
    gr_out.wait()
    for k in range(chips):
        remote(turned.at[k], turned_other.at[k], g_sems, (k,), y_peer).wait_send()
    for slot in range(1, 8):
        for side in (0, 1):
            gather(att_v, slot, side, core_peer).wait_send()
    for kind in (0, 1):
        for delta in range(1, 8):
            remote(
                turned.at[0, 0:own_rows, :],
                pieces.at[kind, :, 0:rows],
                piece_sems,
                (kind, delta),
                core_peer,
            ).wait_send()


def trunk(groups, mask, gain, res, ups, rg, weight, q, k, v):
    rows, width = q.shape
    model = weight.shape[0]
    chips = 4
    part = width // chips
    own_rows = part // 2
    two = 2 * HEAD_DIM
    anywhere = pl.BlockSpec(memory_space=pl.ANY)
    local = pl.BlockSpec(memory_space=pltpu.VMEM)
    low = jnp.bfloat16
    act = jax.ShapeDtypeStruct((rows, width), low)
    dma = pltpu.SemaphoreType.DMA
    return pl.pallas_call(
        functools.partial(trunk_kernel, groups),
        in_specs=[local] * 2 + [anywhere] * 7,
        out_specs=[anywhere] * 7 + [local, anywhere],
        out_shape=[act] * 5
        + [
            jax.ShapeDtypeStruct((own_rows, width), jnp.float32),
            jax.ShapeDtypeStruct((chips, own_rows, part), low),
            jax.ShapeDtypeStruct((width,), jnp.float32),
            jax.ShapeDtypeStruct((8, rows, width), low),
        ],
        scratch_shapes=[
            pltpu.VMEM((rows, width), low),
            pltpu.VMEM((width // HEAD_DIM, rows, rows), low),
            pltpu.VMEM((rows, width), low),
            pltpu.VMEM((rows, width), low),
            pltpu.VMEM((1, width), jnp.float32),
            pltpu.VMEM((chips, rows, part), low),
            pltpu.VMEM((chips, rows, part), low),
            pltpu.VMEM((rows, width), low),
            pltpu.VMEM((rows, width), low),
            pltpu.VMEM((chips, part, rows), low),
            pltpu.VMEM((chips, part, rows), low),
            pltpu.VMEM((rows, part), low),
            pltpu.VMEM((width, width), low),
            pltpu.VMEM((rows, width), jnp.float32),
            pltpu.VMEM((2, own_rows, 8 * rows), low),
            pltpu.VMEM((8, rows), jnp.float32),
            pltpu.VMEM((8, rows), jnp.float32),
            pltpu.VMEM((groups, 1, width), jnp.float32),
            pltpu.VMEM((chips, own_rows, part), low),
            dma((4,)),
            dma((chips,)),
            dma((2, chips)),
            dma((2, chips)),
            dma((2, 1)),
            dma((2, 8, 2)),
            dma((2, 2, 8)),
            dma((2, groups)),
            dma((2, chips)),
            dma((2, 8)),
            dma((2, 4)),
            dma((2, 3)),
            dma((chips,)),
        ],
        compiler_params=pltpu.CompilerParams(
            collective_id=0, has_side_effects=True, vmem_limit_bytes=66 * 1000 * 1000
        ),
        name="trunk",
    )(mask, gain, res, ups, rg, weight, q, k, v)


def hand_out_kernel(*refs):
    for a, b in zip(refs[:5], refs[7:12]):
        b[...] = a[...]
    refs[12][...] = refs[5][...] + refs[6][...].astype(jnp.float32)


def hand_out(arrays, kept, arrived):
    rows, width = arrays[0].shape
    own_rows = kept.shape[0]
    steps, part = arrived.shape[0], arrived.shape[2]
    act = pl.BlockSpec((rows // steps, width), lambda i: (i, 0))
    column = pl.BlockSpec((own_rows, part), lambda i: (0, i))
    return pl.pallas_call(
        hand_out_kernel,
        grid=(steps,),
        in_specs=[act] * 5 + [column, pl.BlockSpec((None, own_rows, part), lambda i: (i, 0, 0))],
        out_specs=[act] * 5 + [column],
        out_shape=[jax.ShapeDtypeStruct((rows, width), jnp.bfloat16)] * 5
        + [jax.ShapeDtypeStruct((own_rows, width), jnp.float32)],
        name="hand_out",
    )(*arrays, kept, arrived)


def sum_groups(groups, value):
    if groups & (groups - 1):
        return lax.psum(value, "dp")
    bit = 1
    while bit < groups:
        value = value + lax.ppermute(value, "dp", [(i, i ^ bit) for i in range(groups)])
        bit *= 2
    return value


def shards(
    groups,
    tensor_size,
    query_rows,
    key_rows,
    value_rows,
    action_mask,
    residual,
    out_weight,
    norm_gain,
    upstream,
    residual_grad,
):
    model_width = out_weight.shape[0]
    own_width = residual.shape[1]
    pair = tensor_size == 2
    swap = [(0, 1), (1, 0)]
    mine = lax.axis_index("tensor")

    def weight_rows(index):
        return lax.dynamic_slice_in_dim(out_weight, index * own_width, own_width, 0)

    def sum_pair(value):
        if pair:
            return value + lax.ppermute(value, "tensor", swap)
        return lax.psum(value, "tensor")

    if pair and groups == 16 and query_rows.shape[0] == LEN:
        out = trunk(
            groups,
            action_mask,
            norm_gain,
            residual,
            upstream,
            residual_grad,
            out_weight,
            query_rows,
            key_rows,
            value_rows,
        )
        return (*hand_out(out[:5], out[5], out[6]), out[7])
    observed = jnp.sum((action_mask == 0).astype(jnp.int32), axis=1)
    probs, attended = attend(observed, query_rows, key_rows, value_rows)
    attended_all = lax.all_gather(attended, "dp", axis=0, tiled=True)
    if pair:
        theirs = dot(attended, weight_rows(1 - mine), NT).astype(jnp.bfloat16)
        arriving = lax.ppermute(theirs, "tensor", swap)
        own = dot(attended, weight_rows(mine), NT)
        own_sum = own + arriving.astype(jnp.float32)
    else:
        own_sum = lax.psum_scatter(
            dot(attended, out_weight, NT), "tensor", scatter_dimension=1, tiled=True
        )
    layer_out = (own_sum + residual.astype(jnp.float32)).astype(jnp.bfloat16)
    out_float = layer_out.astype(jnp.float32)
    upstream_float = upstream.astype(jnp.float32)
    scaled = upstream_float * norm_gain[None, :]
    sums = sum_pair(
        jnp.stack([jnp.sum(out_float * out_float, axis=1), jnp.sum(scaled * out_float, axis=1)])
    )
    row_rms = jnp.sqrt(sums[0] / model_width + epsilon)[:, None]
    normed = out_float / row_rms
    row_inner = sums[1][:, None] / (row_rms * model_width)
    grad_residual = (
        residual_grad.astype(jnp.float32) + (scaled - normed * row_inner) / row_rms
    ).astype(jnp.bfloat16)
    if pair:
        other = lax.ppermute(grad_residual, "tensor", swap)
        first = mine == 0
        low_half = jnp.where(first, grad_residual, other)
        high_half = jnp.where(first, other, grad_residual)
        grad_full = jnp.concatenate([low_half, high_half], axis=1)
        grad_attended = jnp.dot(
            grad_residual, weight_rows(mine), preferred_element_type=jnp.float32
        ) + jnp.dot(other, weight_rows(1 - mine), preferred_element_type=jnp.float32)
    else:
        grad_full = lax.all_gather(grad_residual, "tensor", axis=1, tiled=True)
        grad_attended = jnp.dot(grad_full, out_weight, preferred_element_type=jnp.float32)
    grad_attended = grad_attended.astype(jnp.bfloat16)
    received = lax.all_to_all(grad_full, "dp", split_axis=1, concat_axis=0, tiled=True)
    gain_part = jnp.sum(upstream_float * normed, axis=0)
    grad_query, grad_key, grad_value = attend_backward(
        probs, query_rows, key_rows, value_rows, grad_attended
    )
    grad_query, gain_part = lax.optimization_barrier((grad_query, gain_part))
    grad_gain = sum_groups(groups, gain_part)
    grad_out_weight = dot(received, attended_all, TN)
    return layer_out, grad_residual, grad_query, grad_key, grad_value, grad_out_weight, grad_gain


def solution(mesh):
    rows = P("dp", "tensor")
    return jax.shard_map(
        functools.partial(shards, mesh.shape["dp"], mesh.shape["tensor"]),
        mesh=mesh,
        in_specs=(
            rows,
            rows,
            rows,
            P("dp", None),
            rows,
            P(None, "tensor"),
            P("tensor"),
            rows,
            rows,
        ),
        out_specs=(rows, rows, rows, rows, rows, rows, P("tensor")),
        check_vma=False,
    )
```
